32 devices in a mesh: seq: 16 (over z, y, x), rep: 2 (over core).
Axes of the slice: x: 2, y: 2, z: 4, core: 2. Of those that a mesh axis runs over, the one named last changes fastest.
Arguments:
- tokens: bfloat16 [4, 48, 180, 768], P('rep', 'seq'), may hold values from -6 to 6
- cotangent: bfloat16 [4, 48, 180, 768], P('rep', 'seq'), may hold values from -6 to 6
- in_weight: bfloat16 [2, 8, 96, 96], replicated, may hold values from -0.21875 to 0.21875
- in_bias: float32 [2, 768], replicated, may hold values from -0.6 to 0.6
- out_weight: bfloat16 [2, 8, 96, 96], replicated, may hold values from -0.21875 to 0.21875
- out_bias: float32 [2, 768], replicated, may hold values from -0.12 to 0.12
Outputs:
- mixed_out: bfloat16 [4, 48, 180, 768], P('rep', 'seq')
- tokens_grad: bfloat16 [4, 48, 180, 768], P('rep', 'seq')
- in_weight_grad: float32 [2, 8, 96, 96], replicated
- in_bias_grad: float32 [2, 768], replicated
- out_weight_grad: float32 [2, 8, 96, 96], replicated
- out_bias_grad: float32 [2, 768], replicated
The draws below stay inside these ranges and needn't reach their ends.
All inputs are finite; a program needn't handle non-finite values.
Results may differ from the reference program's by a relative error of at most 0.0094.
Values may be sent and summed in bfloat16 or wider, within the bound.
No kernel may reach another device: no remote copies, remote signals or barrier semaphores. Data moves between devices by JAX's collectives and lax.ppermute only.
A program may use at most 64 MiB of HBM per device.

```python
import math
import jax
import jax.numpy as jnp
from jax import lax

D = 768
BLOCKS = 8
BLOCK = 96
COLS = 180
MODES = 64
ROWS = 48
BATCH = 4


def shard_levels(key, extent, cuts, low, largest):
    def one(axis_at, shards_of):
        heights = jax.random.uniform(jax.random.fold_in(jax.random.fold_in(key, 6), axis_at), (shards_of,), jnp.float32, low / len(cuts), largest / len(cuts))
        return jnp.repeat(jnp.exp(heights), extent[axis_at] // shards_of).reshape((-1,) + (1,) * (len(extent) - axis_at - 1))

    factor_of = one(*cuts[0])
    for cut in cuts[1:]:
        factor_of = factor_of * one(*cut)
    return factor_of


def scatter_about(key, dims, width, limit, pieces=(), kind=jnp.bfloat16):
    drawn = width * jax.random.normal(key, dims, jnp.float32)
    if pieces:
        drawn = drawn * shard_levels(key, dims, pieces, -0.22, 0.18)
    return jnp.clip(drawn, -limit, limit).astype(kind)


def setup_inputs(seed: int = 0) -> dict:
    splits = jax.random.split(jax.random.key(seed), 7)
    tokens = scatter_about(splits[0], (BATCH, ROWS, COLS, D), 1.0, 6.0, ((0, 2), (1, 16)))
    cotangent = scatter_about(splits[1], (BATCH, ROWS, COLS, D), 1.0, 6.0, ((0, 2), (1, 16)))
    in_weight = scatter_about(splits[2], (2, BLOCKS, BLOCK, BLOCK), (8 * BLOCK) ** -0.5, 0.21875)
    in_bias = scatter_about(splits[3], (2, D), 0.1, 0.6, (), jnp.float32)
    out_weight = scatter_about(splits[4], (2, BLOCKS, BLOCK, BLOCK), (8 * BLOCK) ** -0.5, 0.21875)
    out_bias = scatter_about(splits[5], (2, D), 0.02, 0.12, (), jnp.float32)
    return {"tokens": tokens, "cotangent": cotangent, "in_weight": in_weight, "in_bias": in_bias, "out_weight": out_weight, "out_bias": out_bias}


def widen(operand):
    return operand.astype(jnp.float32)

def grid_tables(length, modes):
    position = jnp.arange(length, dtype=jnp.int32)
    frequency = jnp.arange(modes, dtype=jnp.int32)
    residue = position[:, None] * frequency[None, :] % length
    angles = residue.astype(jnp.float32) * (2.0 * math.pi / length)
    factor = 1.0 / math.sqrt(length)
    cosine_table = (jnp.cos(angles) * factor).astype(jnp.bfloat16)
    sine_table = (jnp.sin(angles) * factor).astype(jnp.bfloat16)
    return (cosine_table, sine_table)

def column_tables(grid_width, modes):
    cosine_table, sine_table = grid_tables(grid_width, modes)
    forward = jnp.stack([cosine_table, -sine_table], axis=2)
    doubling = jnp.where(jnp.arange(modes) == 0, 1.0, 2.0).astype(jnp.bfloat16)[:, None]
    inverse = jnp.stack([cosine_table.T * doubling, -(sine_table.T * doubling)], axis=1)
    return (forward, inverse)

def row_table(length):
    cosine_table, sine_table = grid_tables(length, length)
    upper_rows = jnp.stack([cosine_table, sine_table], axis=2)
    lower_rows = jnp.stack([-sine_table, cosine_table], axis=2)
    return jnp.stack([upper_rows, lower_rows], axis=1)

def block_weights(weight):
    real_part, imag_part = (weight[0], weight[1])
    upper_half = jnp.stack([real_part, imag_part], axis=2)
    lower_half = jnp.stack([-imag_part, real_part], axis=2)
    return jnp.stack([upper_half, lower_half], axis=1)

def fold_blocks(blockwise):
    real_part = blockwise[:, 0, :, 0, :] + blockwise[:, 1, :, 1, :]
    imag_part = blockwise[:, 0, :, 1, :] - blockwise[:, 1, :, 0, :]
    return jnp.stack([real_part, imag_part])

def reference(tokens, cotangent, in_weight, in_bias, out_weight, out_bias):
    column_forward, column_inverse = column_tables(COLS, MODES)
    row_matrix = row_table(ROWS)
    weights_in = block_weights(in_weight)
    weights_out = block_weights(out_weight)
    bias_in = in_bias.reshape(2, BLOCKS, BLOCK)
    bias_out = out_bias.reshape(2, BLOCKS, BLOCK)
    mode_count = ROWS * MODES

    def one_sample(pair):
        sample_tokens, sample_cotangent = pair
        spec_rows = jnp.einsum('hwd,wkc->hkcd', widen(sample_tokens), widen(column_forward)).astype(jnp.bfloat16)
        spectrum = jnp.einsum('qehc,hkcd->qked', widen(row_matrix), widen(spec_rows)).astype(jnp.bfloat16)
        flat_modes = spectrum.reshape(mode_count, 2, BLOCKS, BLOCK)
        hidden_pre = jnp.einsum('mcbi,bciej->mebj', widen(flat_modes), widen(weights_in)) + bias_in
        hidden = jax.nn.gelu(hidden_pre).astype(jnp.bfloat16)
        spectrum_out = (jnp.einsum('mcbi,bciej->mebj', widen(hidden), widen(weights_out)) + bias_out).astype(jnp.bfloat16)
        back_rows = jnp.einsum('qehc,qked->hkcd', widen(row_matrix), widen(spectrum_out.reshape(ROWS, MODES, 2, D))).astype(jnp.bfloat16)
        mixed = (widen(sample_tokens) + jnp.einsum('hkcd,kcw->hwd', widen(back_rows), widen(column_inverse))).astype(jnp.bfloat16)
        cot_rows = jnp.einsum('hwd,kcw->hkcd', widen(sample_cotangent), widen(column_inverse)).astype(jnp.bfloat16)
        incoming = jnp.einsum('qehc,hkcd->qked', widen(row_matrix), widen(cot_rows)).astype(jnp.bfloat16)
        incoming = incoming.reshape(mode_count, 2, BLOCKS, BLOCK)
        out_bias_part = lax.optimization_barrier(jnp.sum(widen(incoming), axis=0)).reshape(2, D)
        out_weight_part = fold_blocks(jnp.einsum('mcbi,mebj->bciej', widen(hidden), widen(incoming)))
        hidden_grad = jnp.einsum('mebj,bciej->mcbi', widen(incoming), widen(weights_out))
        pre_grad = jax.vjp(jax.nn.gelu, hidden_pre)[1](hidden_grad)[0].astype(jnp.bfloat16)
        in_bias_part = lax.optimization_barrier(jnp.sum(widen(pre_grad), axis=0)).reshape(2, D)
        in_weight_part = fold_blocks(jnp.einsum('mcbi,mebj->bciej', widen(flat_modes), widen(pre_grad)))
        spectrum_grad = jnp.einsum('mebj,bciej->mcbi', widen(pre_grad), widen(weights_in)).astype(jnp.bfloat16)
        rows_grad = jnp.einsum('qehc,qked->hkcd', widen(row_matrix), widen(spectrum_grad.reshape(ROWS, MODES, 2, D))).astype(jnp.bfloat16)
        grad_tokens = (widen(sample_cotangent) + jnp.einsum('hkcd,wkc->hwd', widen(rows_grad), widen(column_forward))).astype(jnp.bfloat16)
        return (mixed, grad_tokens, in_weight_part, in_bias_part, out_weight_part, out_bias_part)
    outcome = lax.map(one_sample, (tokens, cotangent))
    return (outcome[0], outcome[1], lax.optimization_barrier(jnp.sum(outcome[2], axis=0)) / BATCH, lax.optimization_barrier(jnp.sum(outcome[3], axis=0)) / BATCH, lax.optimization_barrier(jnp.sum(outcome[4], axis=0)) / BATCH, lax.optimization_barrier(jnp.sum(outcome[5], axis=0)) / BATCH)
```

```python
import functools
import math

import jax
import jax.numpy as jnp
import numpy as np
from jax import lax
from jax.experimental import pallas as pl
from jax.experimental.pallas import tpu as pltpu
from jax.sharding import PartitionSpec as P

BLOCKS = 8
BLOCK = 96
MODES = 64
HALVES = 2
HALF = BLOCKS // HALVES * BLOCK
GROUPS = 8
GROUP = MODES // GROUPS
CK = 2 * GROUP
F32 = jnp.float32
BF16 = jnp.bfloat16


def grid_tables(length, modes):
    position = np.arange(length)
    frequency = np.arange(modes)
    residue = position[:, None] * frequency[None, :] % length
    angles = residue.astype(np.float32) * np.float32(2.0 * math.pi / length)
    factor = np.float32(1.0 / math.sqrt(length))
    cosine = (np.cos(angles) * factor).astype(np.float32).astype(BF16)
    sine = (np.sin(angles) * factor).astype(np.float32).astype(BF16)
    return cosine.astype(np.float32), sine.astype(np.float32)


def column_tables(width):
    cosine, sine = grid_tables(width, MODES)
    table = np.stack([cosine.T, -sine.T])
    doubling = np.where(np.arange(MODES) == 0, 1.0, 2.0).astype(np.float32)
    doubled = table * doubling[None, :, None]

    def order(t):
        t = t.reshape(2, GROUPS, GROUP, width).transpose(1, 0, 2, 3)
        return t.reshape(2 * MODES, width)

    return order(table), order(doubled)


def row_matrix(length):
    cosine, sine = grid_tables(length, length)
    small = np.stack(
        [np.stack([cosine.T, sine.T], axis=2), np.stack([-sine.T, cosine.T], axis=2)]
    )
    full = np.zeros((2, length, GROUP, length, 2, GROUP), np.float32)
    for k in range(GROUP):
        full[:, :, k, :, :, k] = small
    size = length * CK
    return full.reshape(size, size)


def dot(a, b):
    return lax.dot_general(a, b, (((1,), (0,)), ((), ())), preferred_element_type=F32)


def dot_t(a, b):
    return lax.dot_general(a, b, (((0,), (0,)), ((), ())), preferred_element_type=F32)


def far(*arrays):
    return [pltpu.with_memory_space_constraint(x, pltpu.HBM) for x in arrays]


def params(limit):
    return pltpu.CompilerParams(vmem_limit_bytes=limit * 1024 * 1024)


def cost(us):
    return pl.CostEstimate(flops=int(us * 2e8), bytes_accessed=int(us * 1e6), transcendentals=0)


def columns_kernel(x_ref, t_ref, o_ref):
    y = dot(t_ref[...], x_ref[0, 0]).astype(BF16)
    for half in range(HALVES):
        part = y[:, half * HALF : (half + 1) * HALF]
        o_ref[half, 0, :, 0] = part.reshape(GROUPS, CK, HALF)


def tile_spec(rows, local):
    return pl.BlockSpec(
        (HALVES, 1, GROUPS, 1, CK, HALF),
        lambda s, h: (0, s // local, 0, (s % local) * rows + h, 0, 0),
    )


def columns(x, table, dims):
    samples, rows, width, channels = x.shape
    split, local = dims
    return pl.pallas_call(
        columns_kernel,
        grid=(samples, rows),
        in_specs=[
            pl.BlockSpec((1, 1, width, channels), lambda s, h: (s, h, 0, 0)),
            pl.BlockSpec((2 * MODES, width), lambda s, h: (0, 0)),
        ],
        out_specs=tile_spec(rows, local),
        out_shape=pltpu.HBM((HALVES, split, GROUPS, local * rows, CK, HALF), BF16),
        compiler_params=params(6),
        cost_estimate=cost(3),
        name="columns",
    )(x, table)


def inverse_kernel(x_ref, t_ref, z_ref, o_ref):
    z = jnp.concatenate(
        [z_ref[half, 0, :, 0].reshape(2 * MODES, HALF) for half in range(HALVES)], axis=1
    )
    o_ref[0, 0] = (x_ref[0, 0].astype(F32) + dot(t_ref[...], z)).astype(BF16)


def inverse(x, table, z, dims):
    samples, rows, width, channels = x.shape
    whole = pl.BlockSpec((1, 1, width, channels), lambda s, h: (s, h, 0, 0))
    return pl.pallas_call(
        inverse_kernel,
        grid=(samples, rows),
        in_specs=[
            whole,
            pl.BlockSpec((width, 2 * MODES), lambda s, h: (0, 0)),
            tile_spec(rows, dims[1]),
        ],
        out_specs=whole,
        out_shape=jax.ShapeDtypeStruct(x.shape, BF16),
        compiler_params=params(8),
        cost_estimate=cost(4),
        name="inverse",
    )(x, table, z)


def prepare_kernel(half_ref, m_ref, wi_ref, wo_ref, n_ref, *outs):
    del half_ref
    n_ref[...] = m_ref[...].astype(F32).T.astype(BF16)
    row = lax.broadcasted_iota(jnp.int32, (BLOCK, HALF), 0)
    lane = lax.broadcasted_iota(jnp.int32, (BLOCK, HALF), 1)
    for w_ref, f_ref, t_ref in ((wi_ref, outs[0], outs[1]), (wo_ref, outs[2], outs[3])):
        diagonal = []
        for c in range(2):
            pieces = []
            for j in range(HALF // BLOCK):
                place = jnp.where(lane == row + j * BLOCK, 1.0, 0.0).astype(BF16)
                pieces.append(dot(w_ref[c, j], place))
            diagonal.append(jnp.concatenate(pieces, axis=0))
        real, imag = diagonal
        real_t, imag_t = real.T.astype(BF16), imag.T.astype(BF16)
        real, imag = real.astype(BF16), imag.astype(BF16)
        f_ref[:HALF, :HALF] = real
        f_ref[:HALF, HALF:] = imag
        f_ref[HALF:, :HALF] = -imag
        f_ref[HALF:, HALF:] = real
        t_ref[:HALF, :HALF] = real_t
        t_ref[:HALF, HALF:] = -imag_t
        t_ref[HALF:, :HALF] = imag_t
        t_ref[HALF:, HALF:] = real_t


def prepare(half, matrix, in_weight, out_weight):
    size = matrix.shape[0]
    weight = pl.BlockSpec((2, HALF // BLOCK, BLOCK, BLOCK), lambda i, half: (0, half[0], 0, 0))
    square = pl.BlockSpec((size, size), lambda i, half: (0, 0))
    wide = pl.BlockSpec((2 * HALF, 2 * HALF), lambda i, half: (0, 0))
    return pl.pallas_call(
        prepare_kernel,
        grid_spec=pltpu.PrefetchScalarGridSpec(
            num_scalar_prefetch=1,
            grid=(1,),
            in_specs=[square, weight, weight],
            out_specs=[square] + [wide] * 4,
        ),
        out_shape=[pltpu.HBM((size, size), BF16)] + [pltpu.HBM((2 * HALF, 2 * HALF), BF16)] * 4,
        compiler_params=params(24),
        cost_estimate=cost(4),
        name="prepare",
    )(half, matrix, in_weight, out_weight)


SLOPE = math.sqrt(2.0 / math.pi)


def side_by_side(x):
    rows = x.shape[0] // 2
    return jnp.concatenate([x[:rows], x[rows:]], axis=1)


def stacked(x):
    return jnp.concatenate([x[:, :HALF], x[:, HALF:]], axis=0)


def bias_row(ref):
    return jnp.concatenate([ref[0:1, :], ref[1:2, :]], axis=1)


def forward_kernel(
    half_ref, v_ref, m_ref, n_ref, wi_ref, wo_ref, bi_ref, bo_ref, o_ref, s_ref, h_ref, d_ref
):
    del half_ref
    size = m_ref.shape[0]
    spectrum = dot(m_ref[...], v_ref[...].reshape(size, HALF)).astype(BF16)
    s_ref[0] = spectrum
    pre = dot(side_by_side(spectrum), wi_ref[...]) + bias_row(bi_ref)
    square = pre * pre
    tanh = jnp.tanh(SLOPE * (pre + 0.044715 * (square * pre)))
    gate = 0.5 * (1.0 + tanh)
    hidden = (pre * gate).astype(BF16)
    d_ref[0] = gate + 0.5 * pre * (1.0 - tanh * tanh) * (SLOPE * (1.0 + 3 * 0.044715 * square))
    h_ref[0] = stacked(hidden)
    out = (dot(hidden, wo_ref[...]) + bias_row(bo_ref)).astype(BF16)
    back = dot(n_ref[...], stacked(out)).astype(BF16)
    o_ref[...] = back.reshape(o_ref.shape)


def forward(rows, local, half, v, m, n, wi, wo, in_bias, out_bias):
    shards = v.shape[0]
    size = m.shape[0]
    chunk = pl.BlockSpec((shards, rows, CK, HALF), lambda s, half: (0, s, 0, 0))
    square = pl.BlockSpec((size, size), lambda s, half: (0, 0))
    wide = pl.BlockSpec((2 * HALF, 2 * HALF), lambda s, half: (0, 0))
    bias = pl.BlockSpec((2, HALF), lambda s, half: (0, half[0]))
    tall = pl.BlockSpec((1, size, HALF), lambda s, half: (s, 0, 0))
    pair = pl.BlockSpec((1, size // 2, 2 * HALF), lambda s, half: (s, 0, 0))
    return pl.pallas_call(
        forward_kernel,
        grid_spec=pltpu.PrefetchScalarGridSpec(
            num_scalar_prefetch=1,
            grid=(local,),
            in_specs=[chunk, square, square, wide, wide, bias, bias],
            out_specs=[chunk, tall, tall, pair],
        ),
        out_shape=[
            pltpu.HBM(v.shape, BF16),
            pltpu.HBM((local, size, HALF), BF16),
            pltpu.HBM((local, size, HALF), BF16),
            pltpu.HBM((local, size // 2, 2 * HALF), F32),
        ],
        compiler_params=params(32),
        cost_estimate=cost(9),
        name="forward",
    )(half, *far(v, m, n, wi, wo), in_bias, out_bias)


PACK = 256


def outer_parts(p_ref, at, left, right):
    rows = right.shape[0] // 2
    turned = jnp.concatenate([right[rows:], -right[:rows]], axis=0)
    full = dot_t(left, jnp.concatenate([right, turned], axis=1))
    block = lax.broadcasted_iota(jnp.int32, (BLOCK, HALF), 1) // BLOCK
    for c in range(2):
        part = full[:, c * HALF : (c + 1) * HALF]
        packed = part[:BLOCK]
        for j in range(1, HALF // BLOCK):
            packed = jnp.where(block == j, part[j * BLOCK : (j + 1) * BLOCK], packed)
        p_ref[at, c * BLOCK : (c + 1) * BLOCK] += packed
    for c in range(2):
        total = jnp.sum(right[c * rows : (c + 1) * rows].astype(F32), axis=0, keepdims=True)
        p_ref[at, 2 * BLOCK + c : 2 * BLOCK + c + 1] += total


def backward_kernel(
    v_ref, m_ref, n_ref, wi_ref, wo_ref, s_ref, h_ref, d_ref, o_ref, p_ref
):
    size = m_ref.shape[0]

    @pl.when(pl.program_id(0) == 0)
    def _():
        p_ref[...] = jnp.zeros_like(p_ref)

    incoming = dot(m_ref[...], v_ref[...].reshape(size, HALF)).astype(BF16)
    hidden_grad = dot(side_by_side(incoming), wo_ref[...])
    pre_grad = (hidden_grad * d_ref[0]).astype(BF16)
    grad = dot(pre_grad, wi_ref[...]).astype(BF16)
    back = dot(n_ref[...], stacked(grad)).astype(BF16)
    o_ref[...] = back.reshape(o_ref.shape)
    outer_parts(p_ref, 0, s_ref[0], stacked(pre_grad))
    outer_parts(p_ref, 1, h_ref[0], incoming)


def backward(rows, local, v, m, n, wi, wo, spectrum, hidden, slope):
    shards = v.shape[0]
    size = m.shape[0]
    chunk = pl.BlockSpec((shards, rows, CK, HALF), lambda s: (0, s, 0, 0))
    square = pl.BlockSpec((size, size), lambda s: (0, 0))
    wide = pl.BlockSpec((2 * HALF, 2 * HALF), lambda s: (0, 0))
    tall = pl.BlockSpec((1, size, HALF), lambda s: (s, 0, 0))
    pair = pl.BlockSpec((1, size // 2, 2 * HALF), lambda s: (s, 0, 0))
    return pl.pallas_call(
        backward_kernel,
        grid=(local,),
        in_specs=[chunk, square, square, wide, wide, tall, tall, pair],
        out_specs=[chunk, pl.BlockSpec((2, PACK, HALF), lambda s: (0, 0, 0))],
        out_shape=[
            pltpu.HBM((shards, local * rows + 1, CK, HALF), BF16),
            jax.ShapeDtypeStruct((2, PACK, HALF), F32),
        ],
        compiler_params=params(32),
        cost_estimate=cost(9),
        name="backward",
    )(*far(v, m, n, wi, wo, spectrum, hidden, slope))


def unpack_kernel(scale, x_ref, iw_ref, ib_ref, ow_ref, ob_ref):
    per = HALF // BLOCK
    for mat, w_ref, b_ref in ((0, iw_ref, ib_ref), (1, ow_ref, ob_ref)):
        for half in range(HALVES):
            for c in range(2):
                part = x_ref[half, mat, c * BLOCK : (c + 1) * BLOCK].astype(F32) * scale
                for j in range(per):
                    moved = part if j == 0 else pltpu.roll(part, HALF - j * BLOCK, 1)
                    w_ref[c, half * per + j] = moved[:, :BLOCK]
            rows = x_ref[half, mat, 2 * BLOCK : 2 * BLOCK + 16].astype(F32) * scale
            b_ref[:, half * HALF : (half + 1) * HALF] = rows[:2]


def unpack(x, scale):
    weight = jax.ShapeDtypeStruct((2, BLOCKS, BLOCK, BLOCK), F32)
    bias = jax.ShapeDtypeStruct((2, HALVES * HALF), F32)
    return pl.pallas_call(
        functools.partial(unpack_kernel, scale),
        out_shape=[weight, bias, weight, bias],
        compiler_params=params(8),
        cost_estimate=cost(2),
        name="unpack",
    )(x)


def swap(x, axis, size, bit):
    return lax.ppermute(x, axis, [(i, i ^ bit) for i in range(size)])


def bits_below(size):
    return [1 << b for b in range((size - 1).bit_length())]


def shards(tokens, cotangent, in_weight, in_bias, out_weight, out_bias):
    samples, row_count, width, _ = tokens.shape
    seq, rep = lax.axis_size("seq"), lax.axis_size("rep")
    split = seq // (HALVES * GROUPS)
    dims = (split, samples // split)
    at, core = lax.axis_index("seq"), lax.axis_index("rep")
    half = (at // (seq // HALVES)).astype(jnp.int32).reshape(1)
    plain, doubled = column_tables(width)
    matrix = jnp.asarray(row_matrix(row_count * seq), BF16)

    def exchange(x):
        return lax.all_to_all(x.reshape((seq,) + x.shape[-3:]), "seq", 0, 0, tiled=True)

    def tiles(x):
        return x.reshape((HALVES, split, GROUPS) + x.shape[1:])

    received = exchange(columns(tokens, jnp.asarray(plain, BF16), dims))
    cot_rows = columns(cotangent, jnp.asarray(doubled, BF16), dims)
    prepared = prepare(half, matrix, in_weight, out_weight)
    cot_rows, prepared = lax.optimization_barrier((cot_rows, prepared))
    inv_matrix, in_fwd, in_bwd, out_fwd, out_bwd = prepared
    incoming = exchange(cot_rows)
    back, spectrum, hidden, slope = forward(
        row_count, dims[1], half, received, matrix, inv_matrix, in_fwd, out_fwd, in_bias, out_bias
    )
    back = exchange(back)
    grad, packet = backward(
        row_count, dims[1], incoming, matrix, inv_matrix, in_bwd, out_bwd, spectrum, hidden, slope
    )

    piece = packet.reshape(2 * PACK, HALF)
    steps = [(core, b) for b in reversed(bits_below(rep))]
    for index, bit in steps:
        count = piece.shape[0] // 2
        mine = (index // bit) % 2
        kept = lax.dynamic_slice_in_dim(piece, mine * count, count, 0)
        sent = lax.dynamic_slice_in_dim(piece, (1 - mine) * count, count, 0)
        piece = kept + swap(sent, "rep", rep, bit)
    part = piece.shape[0] // seq
    share = piece.astype(BF16).reshape(seq, part, HALF)
    if part < CK:
        share = jnp.pad(share, ((0, 0), (0, CK - part), (0, 0)))
    grad = lax.dynamic_update_slice(grad, share[:, None], (0, grad.shape[1] - 1, 0, 0))
    grad, back = lax.optimization_barrier((grad, back))
    grad = exchange(grad)
    total = grad[:, -1, :part].reshape(HALVES, seq // HALVES, part, HALF)
    total = jnp.sum(total.astype(F32), axis=1).astype(BF16)
    mixed_out = inverse(tokens, jnp.asarray(doubled.T, BF16), tiles(back), dims)
    total, mixed_out = lax.optimization_barrier((total, mixed_out))
    gathered = exchange(jnp.broadcast_to(total[None], (seq,) + total.shape))
    tokens_grad = inverse(cotangent, jnp.asarray(plain.T, BF16), tiles(grad), dims)
    gathered, tokens_grad = lax.optimization_barrier((gathered, tokens_grad))
    piece = gathered.transpose(1, 0, 2, 3).reshape(HALVES, seq * part, HALF)
    for index, bit in reversed(steps):
        other = swap(piece, "rep", rep, bit)
        first = ((index // bit) % 2) == 0
        piece = jnp.concatenate(
            [jnp.where(first, piece, other), jnp.where(first, other, piece)], axis=1
        )
    packets = piece.reshape(HALVES, 2, PACK, HALF)
    gradients = unpack(packets, 1.0 / (samples * rep))
    return (mixed_out, tokens_grad, *gradients)


def solution(mesh):
    in_specs = (P("rep", "seq", None, None), P("rep", "seq", None, None), P(), P(), P(), P())
    out_specs = (P("rep", "seq", None, None), P("rep", "seq", None, None), P(), P(), P(), P())
    return jax.shard_map(shards, mesh=mesh, in_specs=in_specs, out_specs=out_specs, check_vma=False)
```

```python
import functools
import math

import jax
import jax.numpy as jnp
import numpy as np
from jax import lax
from jax.experimental import pallas as pl
from jax.experimental.pallas import tpu as pltpu
from jax.sharding import PartitionSpec as P

BLOCKS = 8
BLOCK = 96
MODES = 64
HALVES = 2
HALF = BLOCKS // HALVES * BLOCK
GROUPS = 8
GROUP = MODES // GROUPS
CK = 2 * GROUP
F32 = jnp.float32
BF16 = jnp.bfloat16


def grid_tables(length, modes):
    position = np.arange(length)
    frequency = np.arange(modes)
    residue = position[:, None] * frequency[None, :] % length
    angles = residue.astype(np.float32) * np.float32(2.0 * math.pi / length)
    factor = np.float32(1.0 / math.sqrt(length))
    cosine = (np.cos(angles) * factor).astype(np.float32).astype(BF16)
    sine = (np.sin(angles) * factor).astype(np.float32).astype(BF16)
    return cosine.astype(np.float32), sine.astype(np.float32)


def column_tables(width, samples):
    cosine, sine = grid_tables(width, MODES)
    table = np.stack([cosine.T, -sine.T])
    doubling = np.where(np.arange(MODES) == 0, 1.0, 2.0).astype(np.float32)
    doubled = table * doubling[None, :, None]

    def ordered(t):
        t = t.reshape(2, GROUPS, GROUP, width).transpose(1, 0, 2, 3).reshape(2 * MODES, width)
        full = np.zeros((samples, 2 * MODES, width, samples), np.float32)
        for s in range(samples):
            full[s, :, :, s] = t
        return full.reshape(samples * 2 * MODES, width * samples)

    return ordered(table), ordered(doubled)


def row_matrix(length):
    cosine, sine = grid_tables(length, length)
    small = np.stack(
        [np.stack([cosine.T, sine.T], axis=2), np.stack([-sine.T, cosine.T], axis=2)]
    )
    full = np.zeros((2, length, GROUP, length, 2, GROUP), np.float32)
    for k in range(GROUP):
        full[:, :, k, :, :, k] = small
    size = length * CK
    return full.reshape(size, size).T


def dot(a, b):
    return lax.dot_general(a, b, (((1,), (0,)), ((), ())), preferred_element_type=F32)


def dot_t(a, b):
    return lax.dot_general(a, b, (((0,), (0,)), ((), ())), preferred_element_type=F32)


def far(*arrays):
    return [pltpu.with_memory_space_constraint(x, pltpu.HBM) for x in arrays]


def params(limit):
    return pltpu.CompilerParams(vmem_limit_bytes=limit * 1024 * 1024)


def cost(us):
    return pl.CostEstimate(flops=int(us * 2e8), bytes_accessed=int(us * 1e6), transcendentals=0)


def half_lanes(half):
    return pl.ds(pl.multiple_of(half * HALF, HALF), HALF)


def column_modes(x_ref, t_ref):
    _, width, samples, channels = x_ref.shape
    return dot(t_ref[...], x_ref[0].reshape(width * samples, channels)).astype(BF16)


def columns_kernel(x_ref, t_ref, o_ref):
    y = column_modes(x_ref, t_ref)
    _, split, _, local = o_ref.shape[:4]
    for s in range(split * local):
        for half in range(HALVES):
            part = y[s * 2 * MODES : (s + 1) * 2 * MODES, half * HALF : (half + 1) * HALF]
            o_ref[half, s // local, :, s % local, 0] = part.reshape(GROUPS, CK, HALF)


def tile_spec(dims):
    split, local = dims
    return pl.BlockSpec(
        (HALVES, split, GROUPS, local, 1, CK, HALF), lambda h: (0, 0, 0, 0, h, 0, 0)
    )


def columns(x, table, dims):
    rows, width, samples, channels = x.shape
    split, local = dims
    return pl.pallas_call(
        columns_kernel,
        grid=(rows,),
        in_specs=[
            pl.BlockSpec((1, width, samples, channels), lambda h: (h, 0, 0, 0)),
            pl.BlockSpec(table.shape, lambda h: (0, 0)),
        ],
        out_specs=tile_spec(dims),
        out_shape=pltpu.HBM((HALVES, split, GROUPS, local, rows, CK, HALF), BF16),
        compiler_params=params(16),
        cost_estimate=cost(3),
        name="columns",
    )(*far(x), table)


def columns_apart_kernel(at_ref, x_ref, t_ref, *refs):
    *outs, y_ref = refs
    y_ref[...] = column_modes(x_ref, t_ref).reshape(y_ref.shape)
    split, local = outs[0].shape[:2]
    for s in range(split * local):
        for a in range(HALVES):
            lanes = half_lanes(a ^ at_ref[1])
            for b in range(GROUPS):
                tile = y_ref[s * GROUPS + (b ^ at_ref[3]), :, lanes]
                outs[GROUPS * a + b][(s // local) ^ at_ref[2], s % local, 0] = tile


def columns_apart(at, x, table, dims):
    rows, width, samples, channels = x.shape
    split, local = dims
    out = pl.BlockSpec((split, local, 1, CK, HALF), lambda h, at: (0, 0, h, 0, 0))
    return pl.pallas_call(
        columns_apart_kernel,
        grid_spec=pltpu.PrefetchScalarGridSpec(
            num_scalar_prefetch=1,
            grid=(rows,),
            in_specs=[
                pl.BlockSpec((1, width, samples, channels), lambda h, at: (h, 0, 0, 0)),
                pl.BlockSpec(table.shape, lambda h, at: (0, 0)),
            ],
            out_specs=[out] * (HALVES * GROUPS),
            scratch_shapes=[pltpu.VMEM((samples * GROUPS, CK, channels), BF16)],
        ),
        out_shape=[pltpu.HBM((split, local, rows, CK, HALF), BF16)] * (HALVES * GROUPS),
        compiler_params=params(16),
        cost_estimate=cost(3),
        name="columns_apart",
    )(at, *far(x), table)


def add_modes(o_ref, x_ref, t_ref, z):
    _, width, samples, channels = x_ref.shape
    x = x_ref[0].reshape(width * samples, channels).astype(F32)
    o_ref[0] = (x + dot(t_ref[...], z)).astype(BF16).reshape(width, samples, channels)


def inverse_kernel(x_ref, t_ref, z_ref, o_ref):
    _, split, _, local = z_ref.shape[:4]
    z = jnp.concatenate(
        [
            jnp.concatenate(
                [
                    z_ref[half, s // local, :, s % local, 0].reshape(2 * MODES, HALF)
                    for half in range(HALVES)
                ],
                axis=1,
            )
            for s in range(split * local)
        ],
        axis=0,
    )
    add_modes(o_ref, x_ref, t_ref, z)


def inverse(x, table, z, dims):
    rows, width, samples, channels = x.shape
    whole = pl.BlockSpec((1, width, samples, channels), lambda h: (h, 0, 0, 0))
    return pl.pallas_call(
        inverse_kernel,
        grid=(rows,),
        in_specs=[whole, pl.BlockSpec(table.shape, lambda h: (0, 0)), tile_spec(dims)],
        out_specs=whole,
        out_shape=pltpu.HBM(x.shape, BF16),
        compiler_params=params(16),
        cost_estimate=cost(4),
        name="inverse",
    )(*far(x), table, *far(z))


def inverse_apart_kernel(at_ref, x_ref, t_ref, *refs):
    *slabs, o_ref, z_ref = refs
    split, local = slabs[0].shape[0], len(slabs) // (HALVES * GROUPS)
    for s in range(split * local):
        for a in range(HALVES):
            lanes = half_lanes(a ^ at_ref[1])
            for b in range(GROUPS):
                slab = slabs[(GROUPS * a + b) * local + s % local]
                tile = slab[(s // local) ^ at_ref[2], 0]
                z_ref[s * GROUPS + (b ^ at_ref[3]), :, lanes] = tile
    add_modes(o_ref, x_ref, t_ref, z_ref[...].reshape(t_ref.shape[1], x_ref.shape[3]))


def inverse_apart(at, x, table, slabs, dims):
    rows, width, samples, channels = x.shape
    split, local = dims
    whole = pl.BlockSpec((1, width, samples, channels), lambda h, at: (h, 0, 0, 0))
    slab = [
        pl.BlockSpec((split, 1, CK, HALF), lambda h, at, l=l: (0, l * rows + h, 0, 0))
        for l in range(local)
    ]
    return pl.pallas_call(
        inverse_apart_kernel,
        grid_spec=pltpu.PrefetchScalarGridSpec(
            num_scalar_prefetch=1,
            grid=(rows,),
            in_specs=[whole, pl.BlockSpec(table.shape, lambda h, at: (0, 0))]
            + slab * len(slabs),
            out_specs=whole,
            scratch_shapes=[pltpu.VMEM((samples * GROUPS, CK, channels), BF16)],
        ),
        out_shape=pltpu.HBM(x.shape, BF16),
        compiler_params=params(16),
        cost_estimate=cost(4),
        name="inverse_apart",
    )(at, *far(x), table, *[y for y in far(*slabs) for _ in range(local)])


def transposed(out_ref, blocks):
    for j in range(0, len(blocks), 8):
        rows = jnp.concatenate([x.astype(F32) for x in blocks[j : j + 8]], axis=0)
        width = rows.shape[0]
        out_ref[:, (j // 8) * width : (j // 8 + 1) * width] = rows.T.astype(BF16)


def prepare_kernel(at_ref, base_ref, wi_ref, wo_ref, m_ref, mx_ref, nx_ref, *outs):
    shards = base_ref.shape[0]
    transposed(m_ref, [base_ref[r] for r in range(shards)])
    for r in range(shards):
        nx_ref[r] = base_ref[r ^ at_ref[0]]
    transposed(mx_ref, [nx_ref[r] for r in range(shards)])
    row = lax.broadcasted_iota(jnp.int32, (BLOCK, HALF), 0)
    lane = lax.broadcasted_iota(jnp.int32, (BLOCK, HALF), 1)
    for w_ref, f_ref, t_ref in ((wi_ref, outs[0], outs[1]), (wo_ref, outs[2], outs[3])):
        diagonal = []
        for c in range(2):
            pieces = []
            for j in range(HALF // BLOCK):
                place = jnp.where(lane == row + j * BLOCK, 1.0, 0.0).astype(BF16)
                pieces.append(dot(w_ref[c, j], place))
            diagonal.append(jnp.concatenate(pieces, axis=0))
        real, imag = diagonal
        real_t, imag_t = real.T.astype(BF16), imag.T.astype(BF16)
        real, imag = real.astype(BF16), imag.astype(BF16)
        f_ref[:HALF, :HALF] = real
        f_ref[:HALF, HALF:] = imag
        f_ref[HALF:, :HALF] = -imag
        f_ref[HALF:, HALF:] = real
        t_ref[:HALF, :HALF] = real_t
        t_ref[:HALF, HALF:] = -imag_t
        t_ref[HALF:, :HALF] = imag_t
        t_ref[HALF:, HALF:] = real_t


def prepare(at, base, in_weight, out_weight):
    blocks, rows, size = base.shape
    weight = pl.BlockSpec((2, HALF // BLOCK, BLOCK, BLOCK), lambda i, at: (0, at[1], 0, 0))
    square = pl.BlockSpec((size, size), lambda i, at: (0, 0))
    stack = pl.BlockSpec((blocks, rows, size), lambda i, at: (0, 0, 0))
    wide = pl.BlockSpec((2 * HALF, 2 * HALF), lambda i, at: (0, 0))
    return pl.pallas_call(
        prepare_kernel,
        grid_spec=pltpu.PrefetchScalarGridSpec(
            num_scalar_prefetch=1,
            grid=(1,),
            in_specs=[stack, weight, weight],
            out_specs=[square, square, stack] + [wide] * 4,
        ),
        out_shape=[pltpu.HBM((size, size), BF16)] * 2
        + [pltpu.HBM((blocks, rows, size), BF16)]
        + [pltpu.HBM((2 * HALF, 2 * HALF), BF16)] * 4,
        compiler_params=params(40),
        cost_estimate=cost(4),
        name="prepare",
    )(at, base, in_weight, out_weight)


SLOPE = math.sqrt(2.0 / math.pi)


def side_by_side(x):
    rows = x.shape[0] // 2
    return jnp.concatenate([x[:rows], x[rows:]], axis=1)


def stacked(x):
    return jnp.concatenate([x[:, :HALF], x[:, HALF:]], axis=0)


def bias_row(ref):
    return jnp.concatenate([ref[0:1, :], ref[1:2, :]], axis=1)


def forward_kernel(
    at_ref, v_ref, m_ref, n_ref, wi_ref, wo_ref, bi_ref, bo_ref, o_ref, s_ref, h_ref, d_ref
):
    del at_ref
    size = m_ref.shape[0]
    spectrum = dot(m_ref[...], v_ref[...].reshape(size, HALF)).astype(BF16)
    s_ref[0] = spectrum
    pre = dot(side_by_side(spectrum), wi_ref[...]) + bias_row(bi_ref)
    square = pre * pre
    tanh = jnp.tanh(SLOPE * (pre + 0.044715 * (square * pre)))
    gate = 0.5 * (1.0 + tanh)
    hidden = (pre * gate).astype(BF16)
    d_ref[0] = gate + 0.5 * pre * (1.0 - tanh * tanh) * (SLOPE * (1.0 + 3 * 0.044715 * square))
    h_ref[0] = stacked(hidden)
    out = (dot(hidden, wo_ref[...]) + bias_row(bo_ref)).astype(BF16)
    back = dot(n_ref[...].reshape(size, size), stacked(out)).astype(BF16)
    o_ref[...] = back.reshape(o_ref.shape)


def forward(rows, local, at, v, m, n, wi, wo, in_bias, out_bias):
    shards = v.shape[0]
    size = m.shape[0]
    chunk = pl.BlockSpec((shards, rows, CK, HALF), lambda s, at: (0, s, 0, 0))
    square = pl.BlockSpec((size, size), lambda s, at: (0, 0))
    stack = pl.BlockSpec(n.shape, lambda s, at: (0, 0, 0))
    wide = pl.BlockSpec((2 * HALF, 2 * HALF), lambda s, at: (0, 0))
    bias = pl.BlockSpec((2, HALF), lambda s, at: (0, at[1]))
    tall = pl.BlockSpec((1, size, HALF), lambda s, at: (s, 0, 0))
    pair = pl.BlockSpec((1, size // 2, 2 * HALF), lambda s, at: (s, 0, 0))
    return pl.pallas_call(
        forward_kernel,
        grid_spec=pltpu.PrefetchScalarGridSpec(
            num_scalar_prefetch=1,
            grid=(local,),
            in_specs=[chunk, square, stack, wide, wide, bias, bias],
            out_specs=[chunk, tall, tall, pair],
        ),
        out_shape=[
            pltpu.HBM(v.shape, BF16),
            pltpu.HBM((local, size, HALF), BF16),
            pltpu.HBM((local, size, HALF), BF16),
            pltpu.HBM((local, size // 2, 2 * HALF), F32),
        ],
        compiler_params=params(40),
        cost_estimate=cost(9),
        name="forward",
    )(at, *far(v, m, n, wi, wo), in_bias, out_bias)


PACK = 256


def outer_parts(p_ref, at, left, right):
    rows = right.shape[0] // 2
    turned = jnp.concatenate([right[rows:], -right[:rows]], axis=0)
    full = dot_t(left, jnp.concatenate([right, turned], axis=1))
    block = lax.broadcasted_iota(jnp.int32, (BLOCK, HALF), 1) // BLOCK
    for c in range(2):
        part = full[:, c * HALF : (c + 1) * HALF]
        packed = part[:BLOCK]
        for j in range(1, HALF // BLOCK):
            packed = jnp.where(block == j, part[j * BLOCK : (j + 1) * BLOCK], packed)
        p_ref[at, c * BLOCK : (c + 1) * BLOCK] += packed
    for c in range(2):
        total = jnp.sum(right[c * rows : (c + 1) * rows].astype(F32), axis=0, keepdims=True)
        p_ref[at, 2 * BLOCK + c : 2 * BLOCK + c + 1] += total


def backward_kernel(at_ref, m_ref, wi_ref, wo_ref, s_ref, h_ref, d_ref, *refs):
    *slabs, g_ref, kept_ref, sent_ref, p_ref = refs

    @pl.when(pl.program_id(0) == 0)
    def _():
        p_ref[...] = jnp.zeros_like(p_ref)

    rows = slabs[0].shape[0] * CK
    v = jnp.concatenate([x[...].reshape(rows, HALF) for x in slabs], axis=0)
    incoming = dot(m_ref[...], v).astype(BF16)
    hidden_grad = dot(side_by_side(incoming), wo_ref[...])
    pre_grad = (hidden_grad * d_ref[0]).astype(BF16)
    outer_parts(p_ref, 0, s_ref[0], stacked(pre_grad))
    outer_parts(p_ref, 1, h_ref[0], incoming)
    g_ref[0] = stacked(dot(pre_grad, wi_ref[...]).astype(BF16))

    @pl.when(pl.program_id(0) == pl.num_programs(0) - 1)
    def _():
        kept_ref[...] = p_ref[at_ref[4]]
        sent_ref[...] = p_ref[1 - at_ref[4]]


def backward(rows, local, at, slabs, m, wi, wo, spectrum, hidden, slope):
    size = m.shape[0]
    slab = pl.BlockSpec((rows, CK, HALF), lambda s, at: (s, 0, 0))
    square = pl.BlockSpec((size, size), lambda s, at: (0, 0))
    wide = pl.BlockSpec((2 * HALF, 2 * HALF), lambda s, at: (0, 0))
    tall = pl.BlockSpec((1, size, HALF), lambda s, at: (s, 0, 0))
    pair = pl.BlockSpec((1, size // 2, 2 * HALF), lambda s, at: (s, 0, 0))
    packet = pl.BlockSpec((PACK, HALF), lambda s, at: (0, 0))
    return pl.pallas_call(
        backward_kernel,
        grid_spec=pltpu.PrefetchScalarGridSpec(
            num_scalar_prefetch=1,
            grid=(local,),
            in_specs=[square, wide, wide, tall, tall, pair] + [slab] * len(slabs),
            out_specs=[tall, packet, packet],
            scratch_shapes=[pltpu.VMEM((2, PACK, HALF), F32)],
        ),
        out_shape=[pltpu.HBM((local, size, HALF), BF16)] + [pltpu.HBM((PACK, HALF), F32)] * 2,
        compiler_params=params(40),
        cost_estimate=cost(9),
        name="backward",
    )(at, *far(m, wi, wo, spectrum, hidden, slope, *slabs))


def rows_back_kernel(at_ref, n_ref, g_ref, kept_ref, other_ref, *outs):
    blocks, rows, size = n_ref.shape
    local = g_ref.shape[0]
    for s in range(local):
        back = dot(n_ref[...].reshape(blocks * rows, size), g_ref[s]).astype(BF16)
        back = back.reshape(blocks, rows // CK, CK, HALF)
        for r in range(blocks):
            outs[r][s * rows // CK : (s + 1) * rows // CK] = back[r]
    for r in range(blocks):
        to = r ^ at_ref[0]
        outs[r][local * rows // CK] = (kept_ref[to] + other_ref[to]).astype(BF16)


def rows_back(at, n, grad, kept, other):
    blocks, rows, _ = n.shape
    local = grad.shape[0]
    return pl.pallas_call(
        rows_back_kernel,
        in_specs=[pl.BlockSpec(memory_space=pltpu.SMEM)] + [pl.BlockSpec()] * 4,
        out_shape=[pltpu.HBM((local * rows // CK + 1, CK, HALF), BF16)] * blocks,
        compiler_params=params(24),
        cost_estimate=cost(4),
        name="rows_back",
    )(at, *far(n, grad, kept, other))


def totals_kernel(at_ref, *refs):
    *shares, o_ref = refs
    count = len(shares) // HALVES
    for a in range(HALVES):
        total = shares[a * count][0].astype(F32)
        for x in shares[a * count + 1 : (a + 1) * count]:
            total = total + x[0].astype(F32)
        total = total.astype(BF16)
        for t in range(len(shares)):
            o_ref[t, a ^ at_ref[1]] = total


def totals(at, slabs):
    last = slabs[0].shape[0] - 1
    share = pl.BlockSpec((1, CK, HALF), lambda i, at: (last, 0, 0))
    shape = (len(slabs), HALVES, CK, HALF)
    return pl.pallas_call(
        totals_kernel,
        grid_spec=pltpu.PrefetchScalarGridSpec(
            num_scalar_prefetch=1,
            grid=(1,),
            in_specs=[share] * len(slabs),
            out_specs=pl.BlockSpec(shape, lambda i, at: (0, 0, 0, 0)),
        ),
        out_shape=pltpu.HBM(shape, BF16),
        compiler_params=params(8),
        cost_estimate=cost(2),
        name="totals",
    )(at, *far(*slabs))


def unpack_kernel(scale, at_ref, x_ref, y_ref, iw_ref, ib_ref, ow_ref, ob_ref, pack_ref):
    per = HALF // BLOCK
    for i, ref in enumerate((x_ref, y_ref)):
        for place in range(ref.shape[0]):
            for half in range(HALVES):
                pack_ref[i ^ at_ref[4], half, place] = ref[place, half].astype(F32) * scale
    for mat, w_ref, b_ref in ((0, iw_ref, ib_ref), (1, ow_ref, ob_ref)):
        for half in range(HALVES):
            part = pack_ref[mat, half].reshape(PACK, HALF)
            for j in range(per):
                moved = part if j == 0 else pltpu.roll(part, HALF - j * BLOCK, 1)
                for c in range(2):
                    w_ref[c, half * per + j] = moved[c * BLOCK : (c + 1) * BLOCK, :BLOCK]
            b_ref[:, half * HALF : (half + 1) * HALF] = part[2 * BLOCK : 2 * BLOCK + 2]


def unpack(at, x, y, scale):
    weight = jax.ShapeDtypeStruct((2, BLOCKS, BLOCK, BLOCK), F32)
    bias = jax.ShapeDtypeStruct((2, HALVES * HALF), F32)
    return pl.pallas_call(
        functools.partial(unpack_kernel, scale),
        in_specs=[pl.BlockSpec(memory_space=pltpu.SMEM)]
        + [pl.BlockSpec(memory_space=pltpu.VMEM)] * 2,
        out_shape=[weight, bias, weight, bias],
        scratch_shapes=[pltpu.VMEM((2, HALVES, x.shape[0], CK, HALF), F32)],
        compiler_params=params(16),
        cost_estimate=cost(2),
        name="unpack",
    )(at, x, y)


def unpack_joined(scale, packets):
    per = HALF // BLOCK
    out = []
    for mat in range(2):
        both = packets[mat].astype(F32) * scale
        weight = both[:, : 2 * BLOCK].reshape(HALVES, 2, BLOCK, per, BLOCK)
        out.append(weight.transpose(1, 0, 3, 2, 4).reshape(2, BLOCKS, BLOCK, BLOCK))
        out.append(both[:, 2 * BLOCK : 2 * BLOCK + 2].transpose(1, 0, 2).reshape(2, -1))
    return out


def swap(x, axis, size, bit):
    return lax.ppermute(x, axis, [(i, i ^ bit) for i in range(size)])


def far_first(seq):
    quarter = max(seq // 4, 1)
    classes = [2, 3, 1, 0] if seq >= 4 else [1, 0]
    spread = [[c * quarter + i for i in range(quarter)] for c in classes]
    far = [r for pair in zip(spread[0], spread[1]) for r in pair]
    return [r for r in far + spread[2] + spread[3] if r]


def bits_below(size):
    return [1 << b for b in range((size - 1).bit_length())]


def program(tokens, cotangent, in_weight, in_bias, out_weight, out_bias):
    samples, rows, width, _ = tokens.shape
    seq, rep = lax.axis_size("seq"), lax.axis_size("rep")
    split = seq // (HALVES * GROUPS)
    dims = (split, samples // split)
    local = dims[1]
    place, core = lax.axis_index("seq"), lax.axis_index("rep")
    at = jnp.stack(
        [
            place,
            place // (seq // HALVES),
            place // GROUPS % split,
            place % GROUPS,
            core // max(rep // 2, 1),
        ]
    ).astype(jnp.int32)
    plain, doubled = column_tables(width, samples)
    tokens, cotangent = (x.transpose(1, 2, 0, 3) for x in (tokens, cotangent))
    base = jnp.asarray(row_matrix(rows * seq).reshape(seq, rows * CK, -1), BF16)

    def table(t):
        return jnp.asarray(t, BF16)

    def exchange(x):
        return lax.all_to_all(x.reshape((seq, -1) + x.shape[-2:]), "seq", 0, 0, tiled=True)

    def apart(slabs):
        out = {0: slabs[0]}
        for r in far_first(seq):
            out[r] = swap(slabs[r], "seq", seq, r)
        return [out[r] for r in range(seq)]

    received = exchange(columns(tokens, table(plain), dims))
    cot = columns_apart(at, cotangent, table(doubled), dims)
    cot = [
        cot[GROUPS * a + b][c].reshape(local * rows, CK, HALF)
        for a in range(2)
        for c in range(split)
        for b in range(GROUPS)
    ]
    incoming = apart(cot)
    matrix, matrix_x, base_x, in_fwd, in_bwd, out_fwd, out_bwd = prepare(
        at, base, in_weight, out_weight
    )
    back, spectrum, hidden, slope = forward(
        rows, local, at, received, matrix, base, in_fwd, out_fwd, in_bias, out_bias
    )
    back = exchange(back)
    grad, kept, sent = backward(
        rows, local, at, incoming, matrix_x, in_bwd, out_bwd, spectrum, hidden, slope
    )

    bits = bits_below(rep)[::-1]
    other = swap(sent, "rep", rep, bits[0]) if bits else jnp.zeros_like(sent)
    for bit in bits[1:]:
        piece = kept + other
        count = piece.shape[0] // 2
        mine = (core // bit) % 2
        kept = lax.dynamic_slice_in_dim(piece, mine * count, count, 0)
        sent = lax.dynamic_slice_in_dim(piece, (1 - mine) * count, count, 0)
        other = swap(sent, "rep", rep, bit)
    part = kept.shape[0] // seq

    def by_place(x):
        x = x.reshape(seq, part, HALF)
        return jnp.pad(x, ((0, 0), (0, CK - part), (0, 0))) if part < CK else x

    grad = apart(rows_back(at, base_x, grad, by_place(kept), by_place(other)))
    mixed_out = inverse(
        tokens,
        table(doubled.T),
        back.reshape(HALVES, split, GROUPS, local, rows, CK, HALF),
        dims,
    )
    total = totals(at, grad)
    gathered = exchange(total)
    slabs = [
        jnp.stack([grad[(a * split + c) * GROUPS + b] for c in range(split)])
        for a in range(2)
        for b in range(GROUPS)
    ]
    tokens_grad = inverse_apart(at, cotangent, table(plain.T), slabs, dims)
    gathered, tokens_grad = lax.optimization_barrier((gathered, tokens_grad))
    scale = 1.0 / (samples * rep)
    if rep == 2 and part == CK:
        gradients = unpack(at, gathered, swap(gathered, "rep", rep, 1), scale)
    else:
        piece = gathered[:, :, :part].transpose(1, 0, 2, 3).reshape(HALVES, seq * part, HALF)
        for bit in bits[::-1]:
            other = swap(piece, "rep", rep, bit)
            first = ((core // bit) % 2) == 0
            piece = jnp.concatenate(
                [jnp.where(first, piece, other), jnp.where(first, other, piece)], axis=1
            )
        packets = piece.reshape(HALVES, 2, PACK, HALF).transpose(1, 0, 2, 3)
        gradients = unpack_joined(scale, packets)
    mixed_out, tokens_grad = (x.transpose(2, 0, 1, 3) for x in (mixed_out, tokens_grad))
    return (mixed_out, tokens_grad, *gradients)


def solution(mesh):
    in_specs = (P("rep", "seq", None, None), P("rep", "seq", None, None), P(), P(), P(), P())
    out_specs = (P("rep", "seq", None, None), P("rep", "seq", None, None), P(), P(), P(), P())
    return jax.shard_map(program, mesh=mesh, in_specs=in_specs, out_specs=out_specs, check_vma=False)
```

```python
import functools
import math

import jax
import jax.numpy as jnp
import numpy as np
from jax import lax
from jax.experimental import pallas as pl
from jax.experimental.pallas import tpu as pltpu
from jax.sharding import PartitionSpec as P

BLOCKS = 8
BLOCK = 96
MODES = 64
HALVES = 2
HALF = BLOCKS // HALVES * BLOCK
GROUPS = 8
GROUP = MODES // GROUPS
CK = 2 * GROUP
F32 = jnp.float32
BF16 = jnp.bfloat16


def grid_tables(length, modes):
    position = np.arange(length)
    frequency = np.arange(modes)
    residue = position[:, None] * frequency[None, :] % length
    angles = residue.astype(np.float32) * np.float32(2.0 * math.pi / length)
    factor = np.float32(1.0 / math.sqrt(length))
    cosine = (np.cos(angles) * factor).astype(np.float32).astype(BF16)
    sine = (np.sin(angles) * factor).astype(np.float32).astype(BF16)
    return cosine.astype(np.float32), sine.astype(np.float32)


def column_tables(width, samples):
    cosine, sine = grid_tables(width, MODES)
    table = np.stack([cosine.T, -sine.T])
    doubling = np.where(np.arange(MODES) == 0, 1.0, 2.0).astype(np.float32)
    doubled = table * doubling[None, :, None]

    def ordered(t):
        t = t.reshape(2, GROUPS, GROUP, width).transpose(1, 0, 2, 3).reshape(2 * MODES, width)
        full = np.zeros((samples, 2 * MODES, width, samples), np.float32)
        for s in range(samples):
            full[s, :, :, s] = t
        return full.reshape(samples * 2 * MODES, width * samples)

    return ordered(table), ordered(doubled)


def row_matrix(length):
    cosine, sine = grid_tables(length, length)
    small = np.stack(
        [np.stack([cosine.T, sine.T], axis=2), np.stack([-sine.T, cosine.T], axis=2)]
    )
    full = np.zeros((2, length, GROUP, length, 2, GROUP), np.float32)
    for k in range(GROUP):
        full[:, :, k, :, :, k] = small
    size = length * CK
    return full.reshape(size, size).T


def dot(a, b):
    return lax.dot_general(a, b, (((1,), (0,)), ((), ())), preferred_element_type=F32)


def dot_t(a, b):
    return lax.dot_general(a, b, (((0,), (0,)), ((), ())), preferred_element_type=F32)


def far(*arrays):
    return [pltpu.with_memory_space_constraint(x, pltpu.HBM) for x in arrays]


def params(limit):
    return pltpu.CompilerParams(vmem_limit_bytes=limit * 1024 * 1024)


def cost(us):
    return pl.CostEstimate(flops=int(us * 2e8), bytes_accessed=int(us * 1e6), transcendentals=0)


def half_lanes(half):
    return pl.ds(pl.multiple_of(half * HALF, HALF), HALF)


def column_modes(x_ref, t_ref):
    _, width, samples, channels = x_ref.shape
    return dot(t_ref[...], x_ref[0].reshape(width * samples, channels)).astype(BF16)


def columns_kernel(x_ref, t_ref, o_ref):
    y = column_modes(x_ref, t_ref)
    _, split, _, local = o_ref.shape[:4]
    for s in range(split * local):
        for half in range(HALVES):
            part = y[s * 2 * MODES : (s + 1) * 2 * MODES, half * HALF : (half + 1) * HALF]
            o_ref[half, s // local, :, s % local, 0] = part.reshape(GROUPS, CK, HALF)


def tile_spec(dims):
    split, local = dims
    return pl.BlockSpec(
        (HALVES, split, GROUPS, local, 1, CK, HALF), lambda h: (0, 0, 0, 0, h, 0, 0)
    )


def columns(x, table, dims):
    rows, width, samples, channels = x.shape
    split, local = dims
    return pl.pallas_call(
        columns_kernel,
        grid=(rows,),
        in_specs=[
            pl.BlockSpec((1, width, samples, channels), lambda h: (h, 0, 0, 0)),
            pl.BlockSpec(table.shape, lambda h: (0, 0)),
        ],
        out_specs=tile_spec(dims),
        out_shape=pltpu.HBM((HALVES, split, GROUPS, local, rows, CK, HALF), BF16),
        compiler_params=params(16),
        cost_estimate=cost(3),
        name="columns",
    )(*far(x, table))


def columns_apart_kernel(at_ref, x_ref, t_ref, *refs):
    *outs, y_ref = refs
    y_ref[...] = column_modes(x_ref, t_ref).reshape(y_ref.shape)
    split, local = outs[0].shape[:2]
    for s in range(split * local):
        for a in range(HALVES):
            lanes = half_lanes(a ^ at_ref[1])
            for b in range(GROUPS):
                tile = y_ref[s * GROUPS + (b ^ at_ref[3]), :, lanes]
                outs[GROUPS * a + b][(s // local) ^ at_ref[2], s % local, 0] = tile


def columns_apart(at, x, table, dims):
    rows, width, samples, channels = x.shape
    split, local = dims
    out = pl.BlockSpec((split, local, 1, CK, HALF), lambda h, at: (0, 0, h, 0, 0))
    return pl.pallas_call(
        columns_apart_kernel,
        grid_spec=pltpu.PrefetchScalarGridSpec(
            num_scalar_prefetch=1,
            grid=(rows,),
            in_specs=[
                pl.BlockSpec((1, width, samples, channels), lambda h, at: (h, 0, 0, 0)),
                pl.BlockSpec(table.shape, lambda h, at: (0, 0)),
            ],
            out_specs=[out] * (HALVES * GROUPS),
            scratch_shapes=[pltpu.VMEM((samples * GROUPS, CK, channels), BF16)],
        ),
        out_shape=[pltpu.HBM((split, local, rows, CK, HALF), BF16)] * (HALVES * GROUPS),
        compiler_params=params(16),
        cost_estimate=cost(3),
        name="columns_apart",
    )(at, *far(x, table))


def add_modes(o_ref, x_ref, t_ref, z):
    _, width, samples, channels = x_ref.shape
    x = x_ref[0].reshape(width * samples, channels).astype(F32)
    o_ref[0] = (x + dot(t_ref[...], z)).astype(BF16).reshape(width, samples, channels)


def inverse_kernel(x_ref, t_ref, z_ref, o_ref):
    _, split, _, local = z_ref.shape[:4]
    z = jnp.concatenate(
        [
            jnp.concatenate(
                [
                    z_ref[half, s // local, :, s % local, 0].reshape(2 * MODES, HALF)
                    for half in range(HALVES)
                ],
                axis=1,
            )
            for s in range(split * local)
        ],
        axis=0,
    )
    add_modes(o_ref, x_ref, t_ref, z)


def inverse(x, table, z, dims):
    rows, width, samples, channels = x.shape
    whole = pl.BlockSpec((1, width, samples, channels), lambda h: (h, 0, 0, 0))
    return pl.pallas_call(
        inverse_kernel,
        grid=(rows,),
        in_specs=[whole, pl.BlockSpec(table.shape, lambda h: (0, 0)), tile_spec(dims)],
        out_specs=whole,
        out_shape=pltpu.HBM(x.shape, BF16),
        compiler_params=params(16),
        cost_estimate=cost(4),
        name="inverse",
    )(*far(x, table, z))


def inverse_apart_kernel(at_ref, x_ref, t_ref, *refs):
    *slabs, o_ref, z_ref = refs
    split, local = slabs[0].shape[0], len(slabs) // (HALVES * GROUPS)
    for s in range(split * local):
        for a in range(HALVES):
            lanes = half_lanes(a ^ at_ref[1])
            for b in range(GROUPS):
                slab = slabs[(GROUPS * a + b) * local + s % local]
                tile = slab[(s // local) ^ at_ref[2], 0]
                z_ref[s * GROUPS + (b ^ at_ref[3]), :, lanes] = tile
    add_modes(o_ref, x_ref, t_ref, z_ref[...].reshape(t_ref.shape[1], x_ref.shape[3]))


def inverse_apart(at, x, table, slabs, dims):
    rows, width, samples, channels = x.shape
    split, local = dims
    whole = pl.BlockSpec((1, width, samples, channels), lambda h, at: (h, 0, 0, 0))
    slab = [
        pl.BlockSpec((split, 1, CK, HALF), lambda h, at, l=l: (0, l * rows + h, 0, 0))
        for l in range(local)
    ]
    return pl.pallas_call(
        inverse_apart_kernel,
        grid_spec=pltpu.PrefetchScalarGridSpec(
            num_scalar_prefetch=1,
            grid=(rows,),
            in_specs=[whole, pl.BlockSpec(table.shape, lambda h, at: (0, 0))]
            + slab * len(slabs),
            out_specs=whole,
            scratch_shapes=[pltpu.VMEM((samples * GROUPS, CK, channels), BF16)],
        ),
        out_shape=pltpu.HBM(x.shape, BF16),
        compiler_params=params(16),
        cost_estimate=cost(4),
        name="inverse_apart",
    )(at, *far(x, table), *[y for y in far(*slabs) for _ in range(local)])


def transposed(out_ref, blocks):
    for j in range(0, len(blocks), 8):
        rows = jnp.concatenate([x.astype(F32) for x in blocks[j : j + 8]], axis=0)
        width = rows.shape[0]
        out_ref[:, (j // 8) * width : (j // 8 + 1) * width] = rows.T.astype(BF16)


def prepare_kernel(at_ref, base_ref, wi_ref, wo_ref, m_ref, mx_ref, nx_ref, *outs):
    shards = base_ref.shape[0]
    transposed(m_ref, [base_ref[r] for r in range(shards)])
    for r in range(shards):
        nx_ref[r] = base_ref[r ^ at_ref[0]]
    transposed(mx_ref, [nx_ref[r] for r in range(shards)])
    row = lax.broadcasted_iota(jnp.int32, (BLOCK, HALF), 0)
    lane = lax.broadcasted_iota(jnp.int32, (BLOCK, HALF), 1)
    for w_ref, f_ref, t_ref in ((wi_ref, outs[0], outs[1]), (wo_ref, outs[2], outs[3])):
        diagonal = []
        for c in range(2):
            pieces = []
            for j in range(HALF // BLOCK):
                place = jnp.where(lane == row + j * BLOCK, 1.0, 0.0).astype(BF16)
                pieces.append(dot(w_ref[c, j], place))
            diagonal.append(jnp.concatenate(pieces, axis=0))
        real, imag = diagonal
        real_t, imag_t = real.T.astype(BF16), imag.T.astype(BF16)
        real, imag = real.astype(BF16), imag.astype(BF16)
        f_ref[:HALF, :HALF] = real
        f_ref[:HALF, HALF:] = imag
        f_ref[HALF:, :HALF] = -imag
        f_ref[HALF:, HALF:] = real
        t_ref[:HALF, :HALF] = real_t
        t_ref[:HALF, HALF:] = -imag_t
        t_ref[HALF:, :HALF] = imag_t
        t_ref[HALF:, HALF:] = real_t


def prepare(at, base, in_weight, out_weight):
    blocks, rows, size = base.shape
    weight = pl.BlockSpec((2, HALF // BLOCK, BLOCK, BLOCK), lambda i, at: (0, at[1], 0, 0))
    square = pl.BlockSpec((size, size), lambda i, at: (0, 0))
    stack = pl.BlockSpec((blocks, rows, size), lambda i, at: (0, 0, 0))
    wide = pl.BlockSpec((2 * HALF, 2 * HALF), lambda i, at: (0, 0))
    return pl.pallas_call(
        prepare_kernel,
        grid_spec=pltpu.PrefetchScalarGridSpec(
            num_scalar_prefetch=1,
            grid=(1,),
            in_specs=[stack, weight, weight],
            out_specs=[square, square, stack] + [wide] * 4,
        ),
        out_shape=[pltpu.HBM((size, size), BF16)] * 2
        + [pltpu.HBM((blocks, rows, size), BF16)]
        + [pltpu.HBM((2 * HALF, 2 * HALF), BF16)] * 4,
        compiler_params=params(40),
        cost_estimate=cost(4),
        name="prepare",
    )(at, base, in_weight, out_weight)


SLOPE = math.sqrt(2.0 / math.pi)


def side_by_side(x):
    rows = x.shape[0] // 2
    return jnp.concatenate([x[:rows], x[rows:]], axis=1)


def stacked(x):
    return jnp.concatenate([x[:, :HALF], x[:, HALF:]], axis=0)


def bias_row(ref):
    return jnp.concatenate([ref[0:1, :], ref[1:2, :]], axis=1)


def forward_kernel(
    at_ref, v_ref, m_ref, n_ref, wi_ref, wo_ref, bi_ref, bo_ref, o_ref, s_ref, h_ref, d_ref
):
    del at_ref
    size = m_ref.shape[0]
    spectrum = dot(m_ref[...], v_ref[...].reshape(size, HALF)).astype(BF16)
    s_ref[0] = spectrum
    pre = dot(side_by_side(spectrum), wi_ref[...]) + bias_row(bi_ref)
    square = pre * pre
    tanh = jnp.tanh(SLOPE * (pre + 0.044715 * (square * pre)))
    gate = 0.5 * (1.0 + tanh)
    hidden = (pre * gate).astype(BF16)
    d_ref[0] = gate + 0.5 * pre * (1.0 - tanh * tanh) * (SLOPE * (1.0 + 3 * 0.044715 * square))
    h_ref[0] = stacked(hidden)
    out = (dot(hidden, wo_ref[...]) + bias_row(bo_ref)).astype(BF16)
    back = dot(n_ref[...].reshape(size, size), stacked(out)).astype(BF16)
    o_ref[...] = back.reshape(o_ref.shape)


def forward(rows, local, at, v, m, n, wi, wo, in_bias, out_bias):
    shards = v.shape[0]
    size = m.shape[0]
    chunk = pl.BlockSpec((shards, rows, CK, HALF), lambda s, at: (0, s, 0, 0))
    square = pl.BlockSpec((size, size), lambda s, at: (0, 0))
    stack = pl.BlockSpec(n.shape, lambda s, at: (0, 0, 0))
    wide = pl.BlockSpec((2 * HALF, 2 * HALF), lambda s, at: (0, 0))
    bias = pl.BlockSpec((2, HALF), lambda s, at: (0, at[1]))
    tall = pl.BlockSpec((1, size, HALF), lambda s, at: (s, 0, 0))
    pair = pl.BlockSpec((1, size // 2, 2 * HALF), lambda s, at: (s, 0, 0))
    return pl.pallas_call(
        forward_kernel,
        grid_spec=pltpu.PrefetchScalarGridSpec(
            num_scalar_prefetch=1,
            grid=(local,),
            in_specs=[chunk, square, stack, wide, wide, bias, bias],
            out_specs=[chunk, tall, tall, pair],
        ),
        out_shape=[
            pltpu.HBM(v.shape, BF16),
            pltpu.HBM((local, size, HALF), BF16),
            pltpu.HBM((local, size, HALF), BF16),
            pltpu.HBM((local, size // 2, 2 * HALF), F32),
        ],
        compiler_params=params(40),
        cost_estimate=cost(9),
        name="forward",
    )(at, *far(v, m, n, wi, wo, in_bias, out_bias))


PACK = 256


def outer_parts(p_ref, at, left, right):
    rows = right.shape[0] // 2
    turned = jnp.concatenate([right[rows:], -right[:rows]], axis=0)
    full = dot_t(left, jnp.concatenate([right, turned], axis=1))
    block = lax.broadcasted_iota(jnp.int32, (BLOCK, HALF), 1) // BLOCK
    for c in range(2):
        part = full[:, c * HALF : (c + 1) * HALF]
        packed = part[:BLOCK]
        for j in range(1, HALF // BLOCK):
            packed = jnp.where(block == j, part[j * BLOCK : (j + 1) * BLOCK], packed)
        p_ref[at, c * BLOCK : (c + 1) * BLOCK] += packed
    for c in range(2):
        total = jnp.sum(right[c * rows : (c + 1) * rows].astype(F32), axis=0, keepdims=True)
        p_ref[at, 2 * BLOCK + c : 2 * BLOCK + c + 1] += total


def backward_kernel(at_ref, m_ref, wi_ref, wo_ref, s_ref, h_ref, d_ref, *refs):
    *slabs, g_ref, kept_ref, sent_ref, p_ref = refs

    @pl.when(pl.program_id(0) == 0)
    def _():
        p_ref[...] = jnp.zeros_like(p_ref)

    rows = slabs[0].shape[0] * CK
    v = jnp.concatenate([x[...].reshape(rows, HALF) for x in slabs], axis=0)
    incoming = dot(m_ref[...], v).astype(BF16)
    hidden_grad = dot(side_by_side(incoming), wo_ref[...])
    pre_grad = (hidden_grad * d_ref[0]).astype(BF16)
    outer_parts(p_ref, 0, s_ref[0], stacked(pre_grad))
    outer_parts(p_ref, 1, h_ref[0], incoming)
    g_ref[0] = stacked(dot(pre_grad, wi_ref[...]).astype(BF16))

    @pl.when(pl.program_id(0) == pl.num_programs(0) - 1)
    def _():
        kept_ref[...] = p_ref[at_ref[4]]
        sent_ref[...] = p_ref[1 - at_ref[4]]


def backward(rows, local, at, slabs, m, wi, wo, spectrum, hidden, slope):
    size = m.shape[0]
    slab = pl.BlockSpec((rows, CK, HALF), lambda s, at: (s, 0, 0))
    square = pl.BlockSpec((size, size), lambda s, at: (0, 0))
    wide = pl.BlockSpec((2 * HALF, 2 * HALF), lambda s, at: (0, 0))
    tall = pl.BlockSpec((1, size, HALF), lambda s, at: (s, 0, 0))
    pair = pl.BlockSpec((1, size // 2, 2 * HALF), lambda s, at: (s, 0, 0))
    packet = pl.BlockSpec((PACK, HALF), lambda s, at: (0, 0))
    return pl.pallas_call(
        backward_kernel,
        grid_spec=pltpu.PrefetchScalarGridSpec(
            num_scalar_prefetch=1,
            grid=(local,),
            in_specs=[square, wide, wide, tall, tall, pair] + [slab] * len(slabs),
            out_specs=[tall, packet, packet],
            scratch_shapes=[pltpu.VMEM((2, PACK, HALF), F32)],
        ),
        out_shape=[pltpu.HBM((local, size, HALF), BF16)] + [pltpu.HBM((PACK, HALF), F32)] * 2,
        compiler_params=params(40),
        cost_estimate=cost(9),
        name="backward",
    )(at, *far(m, wi, wo, spectrum, hidden, slope, *slabs))


def rows_back_kernel(at_ref, n_ref, g_ref, kept_ref, other_ref, *outs):
    blocks, rows, size = n_ref.shape
    local = g_ref.shape[0]
    for s in range(local):
        back = dot(n_ref[...].reshape(blocks * rows, size), g_ref[s]).astype(BF16)
        back = back.reshape(blocks, rows // CK, CK, HALF)
        for r in range(blocks):
            outs[r][s * rows // CK : (s + 1) * rows // CK] = back[r]
    tiles = local * rows // CK
    for r in range(blocks // HALVES):
        to = (r ^ at_ref[0]) % (blocks // HALVES)
        outs[r][tiles:] = (kept_ref[to] + other_ref[to]).astype(BF16)


def rows_back(at, n, grad, kept, other):
    blocks, rows, _ = n.shape
    tiles = grad.shape[0] * rows // CK
    counts = [tiles + kept.shape[1]] * (blocks // HALVES) + [tiles] * (blocks // HALVES)
    return pl.pallas_call(
        rows_back_kernel,
        in_specs=[pl.BlockSpec(memory_space=pltpu.SMEM)] + [pl.BlockSpec()] * 4,
        out_shape=[pltpu.HBM((count, CK, HALF), BF16) for count in counts],
        compiler_params=params(24),
        cost_estimate=cost(4),
        name="rows_back",
    )(at, *far(n, grad, kept, other))


def totals_kernel(*refs):
    *shares, o_ref = refs
    total = shares[0][...].astype(F32)
    for x in shares[1:]:
        total = total + x[...].astype(F32)
    total = total.astype(BF16)
    for t in range(o_ref.shape[0]):
        o_ref[t] = total


def totals(slabs, tiles):
    extra = slabs[0].shape[0] - tiles
    count = sum(x.shape[0] > tiles for x in slabs)
    shares = [
        pl.BlockSpec((1, CK, HALF), lambda i, t=t: (tiles + t, 0, 0)) for t in range(extra)
    ]
    body = totals_kernel
    if extra > 1:

        def body(*refs):
            *pieces, o_ref = refs
            for t in range(extra):
                totals_kernel(*pieces[t::extra], o_ref.at[:, t : t + 1])

    return pl.pallas_call(
        body,
        grid=(1,),
        in_specs=shares * count,
        out_specs=pl.BlockSpec((len(slabs), extra, CK, HALF), lambda i: (0, 0, 0, 0)),
        out_shape=pltpu.HBM((len(slabs), extra, CK, HALF), BF16),
        compiler_params=params(8),
        cost_estimate=cost(2),
        name="totals",
    )(*[y for y in far(*slabs[:count]) for _ in range(extra)])


def unpack_kernel(scale, at_ref, x_ref, y_ref, iw_ref, ib_ref, ow_ref, ob_ref, pack_ref):
    per = HALF // BLOCK
    for i, ref in enumerate((x_ref, y_ref)):
        count = ref.shape[0] // HALVES
        for half in range(HALVES):
            for place in range(count):
                block = ref[half * count + place].astype(F32) * scale
                pack_ref[i ^ at_ref[4], half, place] = block
    for mat, w_ref, b_ref in ((0, iw_ref, ib_ref), (1, ow_ref, ob_ref)):
        for half in range(HALVES):
            part = pack_ref[mat, half].reshape(PACK, HALF)
            for j in range(per):
                moved = part if j == 0 else pltpu.roll(part, HALF - j * BLOCK, 1)
                for c in range(2):
                    w_ref[c, half * per + j] = moved[c * BLOCK : (c + 1) * BLOCK, :BLOCK]
            b_ref[:, half * HALF : (half + 1) * HALF] = part[2 * BLOCK : 2 * BLOCK + 2]


def unpack(at, x, y, scale):
    weight = jax.ShapeDtypeStruct((2, BLOCKS, BLOCK, BLOCK), F32)
    bias = jax.ShapeDtypeStruct((2, HALVES * HALF), F32)
    return pl.pallas_call(
        functools.partial(unpack_kernel, scale),
        in_specs=[pl.BlockSpec(memory_space=pltpu.SMEM)]
        + [pl.BlockSpec(memory_space=pltpu.VMEM)] * 2,
        out_shape=[weight, bias, weight, bias],
        scratch_shapes=[pltpu.VMEM((2, HALVES, x.shape[0] // HALVES, *x.shape[1:]), F32)],
        compiler_params=params(16),
        cost_estimate=cost(2),
        name="unpack",
    )(at, x, y)


def unpack_joined(scale, packets):
    per = HALF // BLOCK
    out = []
    for mat in range(2):
        both = packets[mat].astype(F32) * scale
        weight = both[:, : 2 * BLOCK].reshape(HALVES, 2, BLOCK, per, BLOCK)
        out.append(weight.transpose(1, 0, 3, 2, 4).reshape(2, BLOCKS, BLOCK, BLOCK))
        out.append(both[:, 2 * BLOCK : 2 * BLOCK + 2].transpose(1, 0, 2).reshape(2, -1))
    return out


def swap(x, axis, size, bit):
    return lax.ppermute(x, axis, [(i, i ^ bit) for i in range(size)])


def bits_below(size):
    return [1 << b for b in range((size - 1).bit_length())]


def program(tokens, cotangent, in_weight, in_bias, out_weight, out_bias):
    samples, rows, width, _ = tokens.shape
    seq, rep = lax.axis_size("seq"), lax.axis_size("rep")
    split = seq // (HALVES * GROUPS)
    dims = (split, samples // split)
    local = dims[1]
    place, core = lax.axis_index("seq"), lax.axis_index("rep")
    at = jnp.stack(
        [
            place,
            place // (seq // HALVES),
            place // GROUPS % split,
            place % GROUPS,
            core // max(rep // 2, 1),
        ]
    ).astype(jnp.int32)
    plain, doubled = column_tables(width, samples)
    tokens, cotangent = (x.transpose(1, 2, 0, 3) for x in (tokens, cotangent))
    base = jnp.asarray(row_matrix(rows * seq).reshape(seq, rows * CK, -1), BF16)

    def table(t):
        return jnp.asarray(t, BF16)

    def exchange(x):
        return lax.all_to_all(x.reshape((seq, -1) + x.shape[-2:]), "seq", 0, 0, tiled=True)

    def apart(slabs):
        out = {0: slabs[0]}
        for r in range(1, seq):
            out[r] = swap(slabs[r], "seq", seq, r)
        return [out[r] for r in range(seq)]

    received = exchange(columns(tokens, table(plain), dims))
    cot = columns_apart(at, cotangent, table(doubled), dims)
    cot = [
        cot[GROUPS * a + b][c].reshape(local * rows, CK, HALF)
        for a in range(2)
        for c in range(split)
        for b in range(GROUPS)
    ]
    incoming = apart(cot)
    matrix, matrix_x, base_x, in_fwd, in_bwd, out_fwd, out_bwd = prepare(
        at, base, in_weight, out_weight
    )
    back, spectrum, hidden, slope = forward(
        rows, local, at, received, matrix, base, in_fwd, out_fwd, in_bias, out_bias
    )
    back = exchange(back)
    grad, kept, sent = backward(
        rows, local, at, incoming, matrix_x, in_bwd, out_bwd, spectrum, hidden, slope
    )

    bits = bits_below(rep)[::-1]
    other = swap(sent, "rep", rep, bits[0]) if bits else jnp.zeros_like(sent)
    for bit in bits[1:]:
        piece = kept + other
        count = piece.shape[0] // 2
        mine = (core // bit) % 2
        kept = lax.dynamic_slice_in_dim(piece, mine * count, count, 0)
        sent = lax.dynamic_slice_in_dim(piece, (1 - mine) * count, count, 0)
        other = swap(sent, "rep", rep, bit)
    part = kept.shape[0] * HALVES // seq
    whole_tiles = part % CK == 0

    def by_place(x):
        x = x.reshape(seq // HALVES, part, HALF)
        x = jnp.pad(x, ((0, 0), (0, -part % CK), (0, 0)))
        return x.reshape(seq // HALVES, -1, CK, HALF)

    grad = apart(rows_back(at, base_x, grad, by_place(kept), by_place(other)))
    near, back = lax.optimization_barrier((grad[: seq // HALVES], back))
    grad = near + grad[seq // HALVES :]
    total = totals(grad, local * rows)
    mixed_out = inverse(
        tokens,
        table(doubled.T),
        back.reshape(HALVES, split, GROUPS, local, rows, CK, HALF),
        dims,
    )
    gathered = exchange(total)
    slabs = [
        jnp.stack([grad[(a * split + c) * GROUPS + b] for c in range(split)])
        for a in range(2)
        for b in range(GROUPS)
    ]
    tokens_grad = inverse_apart(at, cotangent, table(plain.T), slabs, dims)
    gathered, tokens_grad = lax.optimization_barrier((gathered, tokens_grad))
    scale = 1.0 / (samples * rep)
    if rep == 2 and whole_tiles:
        gradients = unpack(at, gathered, swap(gathered, "rep", rep, 1), scale)
    else:
        piece = gathered.reshape(seq, -1, HALF)[:, :part].reshape(HALVES, -1, HALF)
        for bit in bits[::-1]:
            other = swap(piece, "rep", rep, bit)
            first = ((core // bit) % 2) == 0
            piece = jnp.concatenate(
                [jnp.where(first, piece, other), jnp.where(first, other, piece)], axis=1
            )
        packets = piece.reshape(HALVES, 2, PACK, HALF).transpose(1, 0, 2, 3)
        gradients = unpack_joined(scale, packets)
    mixed_out, tokens_grad = (x.transpose(2, 0, 1, 3) for x in (mixed_out, tokens_grad))
    return (mixed_out, tokens_grad, *gradients)


def solution(mesh):
    in_specs = (P("rep", "seq", None, None), P("rep", "seq", None, None), P(), P(), P(), P())
    out_specs = (P("rep", "seq", None, None), P("rep", "seq", None, None), P(), P(), P(), P())
    return jax.shard_map(program, mesh=mesh, in_specs=in_specs, out_specs=out_specs, check_vma=False)
```

```python
import functools
import math

import jax
import jax.numpy as jnp
import numpy as np
from jax import lax
from jax.experimental import pallas as pl
from jax.experimental.pallas import tpu as pltpu
from jax.sharding import PartitionSpec as P

BLOCKS = 8
BLOCK = 96
MODES = 64
HALVES = 2
HALF = BLOCKS // HALVES * BLOCK
GROUPS = 8
GROUP = MODES // GROUPS
CK = 2 * GROUP
PER = HALF // BLOCK
LANES = 128
F32 = jnp.float32
BF16 = jnp.bfloat16


def grid_tables(length, modes):
    position = np.arange(length)
    frequency = np.arange(modes)
    residue = position[:, None] * frequency[None, :] % length
    angles = residue.astype(np.float32) * np.float32(2.0 * math.pi / length)
    factor = np.float32(1.0 / math.sqrt(length))
    cosine = (np.cos(angles) * factor).astype(np.float32).astype(BF16)
    sine = (np.sin(angles) * factor).astype(np.float32).astype(BF16)
    return cosine.astype(np.float32), sine.astype(np.float32)


def column_tables(width, samples):
    cosine, sine = grid_tables(width, MODES)
    table = np.stack([cosine.T, -sine.T])
    doubling = np.where(np.arange(MODES) == 0, 1.0, 2.0).astype(np.float32)
    doubled = table * doubling[None, :, None]

    def ordered(t):
        t = t.reshape(2, GROUPS, GROUP, width).transpose(1, 0, 2, 3).reshape(2 * MODES, width)
        full = np.zeros((samples, 2 * MODES, width, samples), np.float32)
        for s in range(samples):
            full[s, :, :, s] = t
        return full.reshape(samples * 2 * MODES, width * samples)

    return ordered(table), ordered(doubled)


def row_matrix(length):
    cosine, sine = grid_tables(length, length)
    small = np.stack(
        [np.stack([cosine.T, sine.T], axis=2), np.stack([-sine.T, cosine.T], axis=2)]
    )
    full = np.zeros((2, length, GROUP, length, 2, GROUP), np.float32)
    for k in range(GROUP):
        full[:, :, k, :, :, k] = small
    size = length * CK
    return full.reshape(size, size).T


def dot(a, b):
    return lax.dot_general(a, b, (((1,), (0,)), ((), ())), preferred_element_type=F32)


def dot_t(a, b):
    return lax.dot_general(a, b, (((0,), (0,)), ((), ())), preferred_element_type=F32)


def far(*arrays):
    return [pltpu.with_memory_space_constraint(x, pltpu.HBM) for x in arrays]


def params(limit):
    return pltpu.CompilerParams(vmem_limit_bytes=limit * 1024 * 1024)


def cost(us):
    return pl.CostEstimate(flops=int(us * 2e8), bytes_accessed=int(us * 1e6), transcendentals=0)


def half_lanes(half):
    return pl.ds(pl.multiple_of(half * HALF, HALF), HALF)


def column_modes(x_ref, t_ref):
    _, width, samples, channels = x_ref.shape
    return dot(t_ref[...], x_ref[0].reshape(width * samples, channels)).astype(BF16)


def columns_kernel(x_ref, t_ref, o_ref):
    y = column_modes(x_ref, t_ref)
    _, split, _, local = o_ref.shape[:4]
    for s in range(split * local):
        for half in range(HALVES):
            part = y[s * 2 * MODES : (s + 1) * 2 * MODES, half * HALF : (half + 1) * HALF]
            o_ref[half, s // local, :, s % local, 0] = part.reshape(GROUPS, CK, HALF)


def tile_spec(dims):
    split, local = dims
    return pl.BlockSpec(
        (HALVES, split, GROUPS, local, 1, CK, HALF), lambda h: (0, 0, 0, 0, h, 0, 0)
    )


def columns(x, table, dims):
    rows, width, samples, channels = x.shape
    split, local = dims
    return pl.pallas_call(
        columns_kernel,
        grid=(rows,),
        in_specs=[
            pl.BlockSpec((1, width, samples, channels), lambda h: (h, 0, 0, 0)),
            pl.BlockSpec(table.shape, lambda h: (0, 0)),
        ],
        out_specs=tile_spec(dims),
        out_shape=pltpu.HBM((HALVES, split, GROUPS, local, rows, CK, HALF), BF16),
        compiler_params=params(16),
        cost_estimate=cost(3),
        name="columns",
    )(*far(x, table))


def columns_apart_kernel(at_ref, x_ref, t_ref, *refs):
    *outs, y_ref = refs
    y_ref[...] = column_modes(x_ref, t_ref).reshape(y_ref.shape)
    split, local = outs[0].shape[:2]
    for s in range(split * local):
        for a in range(HALVES):
            lanes = half_lanes(a ^ at_ref[1])
            for b in range(GROUPS):
                tile = y_ref[s * GROUPS + (b ^ at_ref[3]), :, lanes]
                outs[GROUPS * a + b][(s // local) ^ at_ref[2], s % local, 0] = tile


def columns_apart(at, x, table, dims):
    rows, width, samples, channels = x.shape
    split, local = dims
    out = pl.BlockSpec((split, local, 1, CK, HALF), lambda h, at: (0, 0, h, 0, 0))
    return pl.pallas_call(
        columns_apart_kernel,
        grid_spec=pltpu.PrefetchScalarGridSpec(
            num_scalar_prefetch=1,
            grid=(rows,),
            in_specs=[
                pl.BlockSpec((1, width, samples, channels), lambda h, at: (h, 0, 0, 0)),
                pl.BlockSpec(table.shape, lambda h, at: (0, 0)),
            ],
            out_specs=[out] * (HALVES * GROUPS),
            scratch_shapes=[pltpu.VMEM((samples * GROUPS, CK, channels), BF16)],
        ),
        out_shape=[pltpu.HBM((split, local, rows, CK, HALF), BF16)] * (HALVES * GROUPS),
        compiler_params=params(16),
        cost_estimate=cost(3),
        name="columns_apart",
    )(at, *far(x, table))


def add_modes(o_ref, x_ref, t_ref, z):
    _, width, samples, channels = x_ref.shape
    x = x_ref[0].reshape(width * samples, channels).astype(F32)
    o_ref[0] = (x + dot(t_ref[...], z)).astype(BF16).reshape(width, samples, channels)


def inverse_kernel(x_ref, t_ref, z_ref, o_ref):
    _, split, _, local = z_ref.shape[:4]
    z = jnp.concatenate(
        [
            jnp.concatenate(
                [
                    z_ref[half, s // local, :, s % local, 0].reshape(2 * MODES, HALF)
                    for half in range(HALVES)
                ],
                axis=1,
            )
            for s in range(split * local)
        ],
        axis=0,
    )
    add_modes(o_ref, x_ref, t_ref, z)


def inverse(x, table, z, dims):
    rows, width, samples, channels = x.shape
    whole = pl.BlockSpec((1, width, samples, channels), lambda h: (h, 0, 0, 0))
    return pl.pallas_call(
        inverse_kernel,
        grid=(rows,),
        in_specs=[whole, pl.BlockSpec(table.shape, lambda h: (0, 0)), tile_spec(dims)],
        out_specs=whole,
        out_shape=pltpu.HBM(x.shape, BF16),
        compiler_params=params(16),
        cost_estimate=cost(4),
        name="inverse",
    )(*far(x, table, z))


def inverse_apart_kernel(at_ref, x_ref, t_ref, *refs):
    *slabs, o_ref, z_ref = refs
    split, local = slabs[0].shape[0], len(slabs) // (HALVES * GROUPS)
    for s in range(split * local):
        for a in range(HALVES):
            lanes = half_lanes(a ^ at_ref[1])
            for b in range(GROUPS):
                slab = slabs[(GROUPS * a + b) * local + s % local]
                tile = slab[(s // local) ^ at_ref[2], 0]
                z_ref[s * GROUPS + (b ^ at_ref[3]), :, lanes] = tile
    add_modes(o_ref, x_ref, t_ref, z_ref[...].reshape(t_ref.shape[1], x_ref.shape[3]))


def inverse_apart(at, x, table, slabs, dims):
    rows, width, samples, channels = x.shape
    split, local = dims
    whole = pl.BlockSpec((1, width, samples, channels), lambda h, at: (h, 0, 0, 0))
    slab = [
        pl.BlockSpec((split, 1, CK, HALF), lambda h, at, l=l: (0, l * rows + h, 0, 0))
        for l in range(local)
    ]
    return pl.pallas_call(
        inverse_apart_kernel,
        grid_spec=pltpu.PrefetchScalarGridSpec(
            num_scalar_prefetch=1,
            grid=(rows,),
            in_specs=[whole, pl.BlockSpec(table.shape, lambda h, at: (0, 0))]
            + slab * len(slabs),
            out_specs=whole,
            scratch_shapes=[pltpu.VMEM((samples * GROUPS, CK, channels), BF16)],
        ),
        out_shape=pltpu.HBM(x.shape, BF16),
        compiler_params=params(16),
        cost_estimate=cost(4),
        name="inverse_apart",
    )(at, *far(x, table), *[y for y in far(*slabs) for _ in range(local)])


def transposed(out_ref, blocks):
    for j in range(0, len(blocks), 8):
        rows = jnp.concatenate([x.astype(F32) for x in blocks[j : j + 8]], axis=0)
        width = rows.shape[0]
        out_ref[:, (j // 8) * width : (j // 8 + 1) * width] = rows.T.astype(BF16)


def prepare_kernel(at_ref, base_ref, wi_ref, wo_ref, m_ref, mx_ref, nx_ref, *outs):
    shards = base_ref.shape[0]
    transposed(m_ref, [base_ref[r] for r in range(shards)])
    for r in range(shards):
        nx_ref[r] = base_ref[r ^ at_ref[0]]
    transposed(mx_ref, [nx_ref[r] for r in range(shards)])
    row = lax.broadcasted_iota(jnp.int32, (BLOCK, LANES), 0)
    lane = lax.broadcasted_iota(jnp.int32, (BLOCK, LANES), 1)
    place = jnp.where(lane == row, 1.0, 0.0).astype(BF16)
    below = jnp.zeros((LANES - BLOCK, LANES), F32)
    for w_ref, f_ref, t_ref in ((wi_ref, outs[0], outs[1]), (wo_ref, outs[2], outs[3])):
        for j in range(PER):
            real, imag = (
                jnp.concatenate([dot(w_ref[c, j], place), below], axis=0) for c in range(2)
            )
            real_t, imag_t = real.T.astype(BF16), imag.T.astype(BF16)
            real, imag = real.astype(BF16), imag.astype(BF16)
            f_ref[j, :LANES, :LANES] = real
            f_ref[j, :LANES, LANES:] = imag
            f_ref[j, LANES:, :LANES] = -imag
            f_ref[j, LANES:, LANES:] = real
            t_ref[j, :LANES, :LANES] = real_t
            t_ref[j, :LANES, LANES:] = -imag_t
            t_ref[j, LANES:, :LANES] = imag_t
            t_ref[j, LANES:, LANES:] = real_t


def prepare(at, base, in_weight, out_weight):
    blocks, rows, size = base.shape
    weight = pl.BlockSpec((2, HALF // BLOCK, BLOCK, BLOCK), lambda i, at: (0, at[1], 0, 0))
    square = pl.BlockSpec((size, size), lambda i, at: (0, 0))
    stack = pl.BlockSpec((blocks, rows, size), lambda i, at: (0, 0, 0))
    wide = pl.BlockSpec((PER, 2 * LANES, 2 * LANES), lambda i, at: (0, 0, 0))
    return pl.pallas_call(
        prepare_kernel,
        grid_spec=pltpu.PrefetchScalarGridSpec(
            num_scalar_prefetch=1,
            grid=(1,),
            in_specs=[stack, weight, weight],
            out_specs=[square, square, stack] + [wide] * 4,
        ),
        out_shape=[pltpu.HBM((size, size), BF16)] * 2
        + [pltpu.HBM((blocks, rows, size), BF16)]
        + [pltpu.HBM((PER, 2 * LANES, 2 * LANES), BF16)] * 4,
        compiler_params=params(40),
        cost_estimate=cost(4),
        name="prepare",
    )(at, base, in_weight, out_weight)


SLOPE = math.sqrt(2.0 / math.pi)


def padded(x):
    blank = jnp.zeros((x.shape[0], LANES - BLOCK), x.dtype)
    pieces = []
    for j in range(PER):
        pieces += [x[:, j * BLOCK : (j + 1) * BLOCK], blank]
    return jnp.concatenate(pieces, axis=1)


def packed(x):
    return jnp.concatenate([x[:, j * LANES : j * LANES + BLOCK] for j in range(PER)], axis=1)


def lanes_of(j):
    return slice(j * LANES, (j + 1) * LANES)


def parts_of(x, j):
    rows = x.shape[0] // 2
    return jnp.concatenate([x[:rows, lanes_of(j)], x[rows:, lanes_of(j)]], axis=1)


def joined(blocks):
    halves = [
        packed(jnp.concatenate([x[:, lanes_of(c)] for x in blocks], axis=1)) for c in range(2)
    ]
    return jnp.concatenate(halves, axis=0)


def bias_row(ref, j):
    return jnp.concatenate([ref[0:1, lanes_of(j)], ref[1:2, lanes_of(j)]], axis=1)


def forward_kernel(
    at_ref, v_ref, m_ref, n_ref, wi_ref, wo_ref, bi_ref, bo_ref, o_ref, s_ref, h_ref, d_ref
):
    del at_ref
    size = m_ref.shape[0]
    rows = size // 2
    spectrum = dot(m_ref[...], padded(v_ref[...].reshape(size, HALF))).astype(BF16)
    s_ref[0] = spectrum
    blocks = []
    for j in range(PER):
        pre = dot(parts_of(spectrum, j), wi_ref[j]) + bias_row(bi_ref, j)
        square = pre * pre
        tanh = jnp.tanh(SLOPE * (pre + 0.044715 * (square * pre)))
        gate = 0.5 * (1.0 + tanh)
        hidden = (pre * gate).astype(BF16)
        rise = SLOPE * (1.0 + 3 * 0.044715 * square)
        d_ref[0, j] = gate + 0.5 * pre * (1.0 - tanh * tanh) * rise
        h_ref[0, :rows, lanes_of(j)] = hidden[:, :LANES]
        h_ref[0, rows:, lanes_of(j)] = hidden[:, LANES:]
        blocks.append((dot(hidden, wo_ref[j]) + bias_row(bo_ref, j)).astype(BF16))
    back = dot(n_ref[...].reshape(size, size), joined(blocks)).astype(BF16)
    o_ref[...] = back.reshape(o_ref.shape)


def forward(rows, local, at, v, m, n, wi, wo, in_bias, out_bias):
    shards = v.shape[0]
    size = m.shape[0]
    chunk = pl.BlockSpec((shards, rows, CK, HALF), lambda s, at: (0, s, 0, 0))
    square = pl.BlockSpec((size, size), lambda s, at: (0, 0))
    stack = pl.BlockSpec(n.shape, lambda s, at: (0, 0, 0))
    wide = pl.BlockSpec((PER, 2 * LANES, 2 * LANES), lambda s, at: (0, 0, 0))
    bias = pl.BlockSpec((2, PER * LANES), lambda s, at: (0, at[1]))
    tall = pl.BlockSpec((1, size, PER * LANES), lambda s, at: (s, 0, 0))
    pair = pl.BlockSpec((1, PER, size // 2, 2 * LANES), lambda s, at: (s, 0, 0, 0))
    return pl.pallas_call(
        forward_kernel,
        grid_spec=pltpu.PrefetchScalarGridSpec(
            num_scalar_prefetch=1,
            grid=(local,),
            in_specs=[chunk, square, stack, wide, wide, bias, bias],
            out_specs=[chunk, tall, tall, pair],
        ),
        out_shape=[
            pltpu.HBM(v.shape, BF16),
            pltpu.HBM((local, size, PER * LANES), BF16),
            pltpu.HBM((local, size, PER * LANES), BF16),
            pltpu.HBM((local, PER, size // 2, 2 * LANES), F32),
        ],
        compiler_params=params(40),
        cost_estimate=cost(9),
        name="forward",
    )(at, *far(v, m, n, wi, wo, in_bias, out_bias))


PACK = 256


def outer_parts(p_ref, at, j, left, right):
    lanes = lanes_of(j)
    turned = jnp.concatenate([right[:, LANES:], -right[:, :LANES]], axis=1)
    full = dot_t(left, jnp.concatenate([right, turned], axis=0))
    sums = jnp.sum(right.astype(F32), axis=0, keepdims=True)
    for c in range(2):
        p_ref[at, c * BLOCK : (c + 1) * BLOCK, lanes] += full[:BLOCK, lanes_of(c)]
        p_ref[at, 2 * BLOCK + c : 2 * BLOCK + c + 1, lanes] += sums[:, lanes_of(c)]


def backward_kernel(at_ref, m_ref, wi_ref, wo_ref, s_ref, h_ref, d_ref, *refs):
    *slabs, g_ref, kept_ref, sent_ref, p_ref = refs

    @pl.when(pl.program_id(0) == 0)
    def _():
        p_ref[...] = jnp.zeros_like(p_ref)

    rows = slabs[0].shape[0] * CK
    v = jnp.concatenate([x[...].reshape(rows, HALF) for x in slabs], axis=0)
    incoming = dot(m_ref[...], padded(v)).astype(BF16)
    blocks = []
    for j in range(PER):
        coming = parts_of(incoming, j)
        pre_grad = (dot(coming, wo_ref[j]) * d_ref[0, j]).astype(BF16)
        blocks.append(dot(pre_grad, wi_ref[j]).astype(BF16))
        outer_parts(p_ref, 0, j, s_ref[0, :, lanes_of(j)], pre_grad)
        outer_parts(p_ref, 1, j, h_ref[0, :, lanes_of(j)], coming)
    g_ref[0] = joined(blocks)

    @pl.when(pl.program_id(0) == pl.num_programs(0) - 1)
    def _():
        kept_ref[...] = packed(p_ref[at_ref[4]])
        sent_ref[...] = packed(p_ref[1 - at_ref[4]])


def backward(rows, local, at, slabs, m, wi, wo, spectrum, hidden, slope):
    size = m.shape[0]
    slab = pl.BlockSpec((rows, CK, HALF), lambda s, at: (s, 0, 0))
    square = pl.BlockSpec((size, size), lambda s, at: (0, 0))
    wide = pl.BlockSpec((PER, 2 * LANES, 2 * LANES), lambda s, at: (0, 0, 0))
    tall = pl.BlockSpec((1, size, PER * LANES), lambda s, at: (s, 0, 0))
    given = pl.BlockSpec((1, size, HALF), lambda s, at: (s, 0, 0))
    pair = pl.BlockSpec((1, PER, size // 2, 2 * LANES), lambda s, at: (s, 0, 0, 0))
    packet = pl.BlockSpec((PACK, HALF), lambda s, at: (0, 0))
    return pl.pallas_call(
        backward_kernel,
        grid_spec=pltpu.PrefetchScalarGridSpec(
            num_scalar_prefetch=1,
            grid=(local,),
            in_specs=[square, wide, wide, tall, tall, pair] + [slab] * len(slabs),
            out_specs=[given, packet, packet],
            scratch_shapes=[pltpu.VMEM((2, PACK, PER * LANES), F32)],
        ),
        out_shape=[pltpu.HBM((local, size, HALF), BF16)] + [pltpu.HBM((PACK, HALF), F32)] * 2,
        compiler_params=params(40),
        cost_estimate=cost(9),
        name="backward",
    )(at, *far(m, wi, wo, spectrum, hidden, slope, *slabs))


def rows_back_kernel(at_ref, n_ref, g_ref, kept_ref, other_ref, *outs):
    blocks, rows, size = n_ref.shape
    local = g_ref.shape[0]
    for s in range(local):
        back = dot(n_ref[...].reshape(blocks * rows, size), g_ref[s]).astype(BF16)
        back = back.reshape(blocks, rows // CK, CK, HALF)
        for r in range(blocks):
            outs[r][s * rows // CK : (s + 1) * rows // CK] = back[r]
    tiles = local * rows // CK
    for r in range(blocks // HALVES):
        to = (r ^ at_ref[0]) % (blocks // HALVES)
        outs[r][tiles:] = (kept_ref[to] + other_ref[to]).astype(BF16)


def rows_back(at, n, grad, kept, other):
    blocks, rows, _ = n.shape
    tiles = grad.shape[0] * rows // CK
    counts = [tiles + kept.shape[1]] * (blocks // HALVES) + [tiles] * (blocks // HALVES)
    return pl.pallas_call(
        rows_back_kernel,
        in_specs=[pl.BlockSpec(memory_space=pltpu.SMEM)] + [pl.BlockSpec()] * 4,
        out_shape=[pltpu.HBM((count, CK, HALF), BF16) for count in counts],
        compiler_params=params(24),
        cost_estimate=cost(4),
        name="rows_back",
    )(at, *far(n, grad, kept, other))


def totals_kernel(*refs):
    *shares, o_ref = refs
    total = shares[0][...].astype(F32)
    for x in shares[1:]:
        total = total + x[...].astype(F32)
    total = total.astype(BF16)
    for t in range(o_ref.shape[0]):
        o_ref[t] = total


def totals(slabs, tiles):
    extra = slabs[0].shape[0] - tiles
    count = sum(x.shape[0] > tiles for x in slabs)
    shares = [
        pl.BlockSpec((1, CK, HALF), lambda i, t=t: (tiles + t, 0, 0)) for t in range(extra)
    ]
    body = totals_kernel
    if extra > 1:

        def body(*refs):
            *pieces, o_ref = refs
            for t in range(extra):
                totals_kernel(*pieces[t::extra], o_ref.at[:, t : t + 1])

    return pl.pallas_call(
        body,
        grid=(1,),
        in_specs=shares * count,
        out_specs=pl.BlockSpec((len(slabs), extra, CK, HALF), lambda i: (0, 0, 0, 0)),
        out_shape=pltpu.HBM((len(slabs), extra, CK, HALF), BF16),
        compiler_params=params(8),
        cost_estimate=cost(2),
        name="totals",
    )(*[y for y in far(*slabs[:count]) for _ in range(extra)])


def unpack_kernel(scale, at_ref, x_ref, y_ref, iw_ref, ib_ref, ow_ref, ob_ref, pack_ref):
    per = HALF // BLOCK
    for i, ref in enumerate((x_ref, y_ref)):
        count = ref.shape[0] // HALVES
        for half in range(HALVES):
            for place in range(count):
                block = ref[half * count + place].astype(F32) * scale
                pack_ref[i ^ at_ref[4], half, place] = block
    for mat, w_ref, b_ref in ((0, iw_ref, ib_ref), (1, ow_ref, ob_ref)):
        for half in range(HALVES):
            part = pack_ref[mat, half].reshape(PACK, HALF)
            for j in range(per):
                moved = part if j == 0 else pltpu.roll(part, HALF - j * BLOCK, 1)
                for c in range(2):
                    w_ref[c, half * per + j] = moved[c * BLOCK : (c + 1) * BLOCK, :BLOCK]
            b_ref[:, half * HALF : (half + 1) * HALF] = part[2 * BLOCK : 2 * BLOCK + 2]


def unpack(at, x, y, scale):
    weight = jax.ShapeDtypeStruct((2, BLOCKS, BLOCK, BLOCK), F32)
    bias = jax.ShapeDtypeStruct((2, HALVES * HALF), F32)
    return pl.pallas_call(
        functools.partial(unpack_kernel, scale),
        in_specs=[pl.BlockSpec(memory_space=pltpu.SMEM)]
        + [pl.BlockSpec(memory_space=pltpu.VMEM)] * 2,
        out_shape=[weight, bias, weight, bias],
        scratch_shapes=[pltpu.VMEM((2, HALVES, x.shape[0] // HALVES, *x.shape[1:]), F32)],
        compiler_params=params(16),
        cost_estimate=cost(2),
        name="unpack",
    )(at, x, y)


def unpack_joined(scale, packets):
    per = HALF // BLOCK
    out = []
    for mat in range(2):
        both = packets[mat].astype(F32) * scale
        weight = both[:, : 2 * BLOCK].reshape(HALVES, 2, BLOCK, per, BLOCK)
        out.append(weight.transpose(1, 0, 3, 2, 4).reshape(2, BLOCKS, BLOCK, BLOCK))
        out.append(both[:, 2 * BLOCK : 2 * BLOCK + 2].transpose(1, 0, 2).reshape(2, -1))
    return out


def swap(x, axis, size, bit):
    return lax.ppermute(x, axis, [(i, i ^ bit) for i in range(size)])


def bits_below(size):
    return [1 << b for b in range((size - 1).bit_length())]


def program(tokens, cotangent, in_weight, in_bias, out_weight, out_bias):
    samples, rows, width, _ = tokens.shape
    seq, rep = lax.axis_size("seq"), lax.axis_size("rep")
    split = seq // (HALVES * GROUPS)
    dims = (split, samples // split)
    local = dims[1]
    place, core = lax.axis_index("seq"), lax.axis_index("rep")
    at = jnp.stack(
        [
            place,
            place // (seq // HALVES),
            place // GROUPS % split,
            place % GROUPS,
            core // max(rep // 2, 1),
        ]
    ).astype(jnp.int32)
    plain, doubled = column_tables(width, samples)
    tokens, cotangent = (x.transpose(1, 2, 0, 3) for x in (tokens, cotangent))
    base = jnp.asarray(row_matrix(rows * seq).reshape(seq, rows * CK, -1), BF16)

    def table(t):
        return jnp.asarray(t, BF16)

    def exchange(x):
        return lax.all_to_all(x.reshape((seq, -1) + x.shape[-2:]), "seq", 0, 0, tiled=True)

    def apart(slabs):
        out = {0: slabs[0]}
        for r in range(1, seq):
            out[r] = swap(slabs[r], "seq", seq, r)
        return [out[r] for r in range(seq)]

    received = exchange(columns(tokens, table(plain), dims))
    cot = columns_apart(at, cotangent, table(doubled), dims)
    cot = [
        cot[GROUPS * a + b][c].reshape(local * rows, CK, HALF)
        for a in range(2)
        for c in range(split)
        for b in range(GROUPS)
    ]
    incoming = apart(cot)
    matrix, matrix_x, base_x, in_fwd, in_bwd, out_fwd, out_bwd = prepare(
        at, base, in_weight, out_weight
    )
    in_bias, out_bias = (
        jnp.pad(x.reshape(2, BLOCKS, BLOCK), ((0, 0), (0, 0), (0, LANES - BLOCK))).reshape(2, -1)
        for x in (in_bias, out_bias)
    )
    back, spectrum, hidden, slope = forward(
        rows, local, at, received, matrix, base, in_fwd, out_fwd, in_bias, out_bias
    )
    back = exchange(back)
    grad, kept, sent = backward(
        rows, local, at, incoming, matrix_x, in_bwd, out_bwd, spectrum, hidden, slope
    )

    bits = bits_below(rep)[::-1]
    other = swap(sent, "rep", rep, bits[0]) if bits else jnp.zeros_like(sent)
    for bit in bits[1:]:
        piece = kept + other
        count = piece.shape[0] // 2
        mine = (core // bit) % 2
        kept = lax.dynamic_slice_in_dim(piece, mine * count, count, 0)
        sent = lax.dynamic_slice_in_dim(piece, (1 - mine) * count, count, 0)
        other = swap(sent, "rep", rep, bit)
    part = kept.shape[0] * HALVES // seq
    whole_tiles = part % CK == 0

    def by_place(x):
        x = x.reshape(seq // HALVES, part, HALF)
        x = jnp.pad(x, ((0, 0), (0, -part % CK), (0, 0)))
        return x.reshape(seq // HALVES, -1, CK, HALF)

    grad = apart(rows_back(at, base_x, grad, by_place(kept), by_place(other)))
    near, back = lax.optimization_barrier((grad[: seq // HALVES], back))
    grad = near + grad[seq // HALVES :]
    total = totals(grad, local * rows)
    mixed_out = inverse(
        tokens,
        table(doubled.T),
        back.reshape(HALVES, split, GROUPS, local, rows, CK, HALF),
        dims,
    )
    gathered = exchange(total)
    slabs = [
        jnp.stack([grad[(a * split + c) * GROUPS + b] for c in range(split)])
        for a in range(2)
        for b in range(GROUPS)
    ]
    tokens_grad = inverse_apart(at, cotangent, table(plain.T), slabs, dims)
    gathered, tokens_grad = lax.optimization_barrier((gathered, tokens_grad))
    scale = 1.0 / (samples * rep)
    if rep == 2 and whole_tiles:
        gradients = unpack(at, gathered, swap(gathered, "rep", rep, 1), scale)
    else:
        piece = gathered.reshape(seq, -1, HALF)[:, :part].reshape(HALVES, -1, HALF)
        for bit in bits[::-1]:
            other = swap(piece, "rep", rep, bit)
            first = ((core // bit) % 2) == 0
            piece = jnp.concatenate(
                [jnp.where(first, piece, other), jnp.where(first, other, piece)], axis=1
            )
        packets = piece.reshape(HALVES, 2, PACK, HALF).transpose(1, 0, 2, 3)
        gradients = unpack_joined(scale, packets)
    mixed_out, tokens_grad = (x.transpose(2, 0, 1, 3) for x in (mixed_out, tokens_grad))
    return (mixed_out, tokens_grad, *gradients)


def solution(mesh):
    in_specs = (P("rep", "seq", None, None), P("rep", "seq", None, None), P(), P(), P(), P())
    out_specs = (P("rep", "seq", None, None), P("rep", "seq", None, None), P(), P(), P(), P())
    return jax.shard_map(program, mesh=mesh, in_specs=in_specs, out_specs=out_specs, check_vma=False)
```

```python
import functools
import math

import jax
import jax.numpy as jnp
import numpy as np
from jax import lax
from jax.experimental import pallas as pl
from jax.experimental.pallas import tpu as pltpu
from jax.sharding import PartitionSpec as P

BLOCKS = 8
BLOCK = 96
MODES = 64
HALVES = 2
HALF = BLOCKS // HALVES * BLOCK
GROUPS = 8
GROUP = MODES // GROUPS
CK = 2 * GROUP
PER = HALF // BLOCK
LANES = 128
F32 = jnp.float32
BF16 = jnp.bfloat16


def grid_tables(length, modes):
    position = np.arange(length)
    frequency = np.arange(modes)
    residue = position[:, None] * frequency[None, :] % length
    angles = residue.astype(np.float32) * np.float32(2.0 * math.pi / length)
    factor = np.float32(1.0 / math.sqrt(length))
    cosine = (np.cos(angles) * factor).astype(np.float32).astype(BF16)
    sine = (np.sin(angles) * factor).astype(np.float32).astype(BF16)
    return cosine.astype(np.float32), sine.astype(np.float32)


def column_tables(width, samples):
    cosine, sine = grid_tables(width, MODES)
    table = np.stack([cosine.T, -sine.T])
    doubling = np.where(np.arange(MODES) == 0, 1.0, 2.0).astype(np.float32)
    doubled = table * doubling[None, :, None]

    def ordered(t):
        t = t.reshape(2, GROUPS, GROUP, width).transpose(1, 0, 2, 3).reshape(2 * MODES, width)
        full = np.zeros((samples, 2 * MODES, width, samples), np.float32)
        for s in range(samples):
            full[s, :, :, s] = t
        return full.reshape(samples * 2 * MODES, width * samples)

    return ordered(table), ordered(doubled)


def row_matrix(length):
    cosine, sine = grid_tables(length, length)
    small = np.stack(
        [np.stack([cosine.T, sine.T], axis=2), np.stack([-sine.T, cosine.T], axis=2)]
    )
    full = np.zeros((2, length, GROUP, length, 2, GROUP), np.float32)
    for k in range(GROUP):
        full[:, :, k, :, :, k] = small
    size = length * CK
    return full.reshape(size, size).T


def dot(a, b):
    return lax.dot_general(a, b, (((1,), (0,)), ((), ())), preferred_element_type=F32)


def dot_t(a, b):
    return lax.dot_general(a, b, (((0,), (0,)), ((), ())), preferred_element_type=F32)


def far(*arrays):
    return [pltpu.with_memory_space_constraint(x, pltpu.HBM) for x in arrays]


def params(limit):
    return pltpu.CompilerParams(vmem_limit_bytes=limit * 1024 * 1024)


def cost(us):
    return pl.CostEstimate(flops=int(us * 2e8), bytes_accessed=int(us * 1e6), transcendentals=0)


def half_lanes(half):
    return pl.ds(pl.multiple_of(half * HALF, HALF), HALF)


def column_modes(x_ref, t_ref):
    _, width, samples, channels = x_ref.shape
    return dot(t_ref[...], x_ref[0].reshape(width * samples, channels)).astype(BF16)


def columns_kernel(x_ref, t_ref, o_ref):
    y = column_modes(x_ref, t_ref)
    _, split, _, local = o_ref.shape[:4]
    for s in range(split * local):
        for half in range(HALVES):
            part = y[s * 2 * MODES : (s + 1) * 2 * MODES, half * HALF : (half + 1) * HALF]
            o_ref[half, s // local, :, s % local, 0] = part.reshape(GROUPS, CK, HALF)


def tile_spec(dims):
    split, local = dims
    return pl.BlockSpec(
        (HALVES, split, GROUPS, local, 1, CK, HALF), lambda h: (0, 0, 0, 0, h, 0, 0)
    )


def columns(x, table, dims):
    rows, width, samples, channels = x.shape
    split, local = dims
    return pl.pallas_call(
        columns_kernel,
        grid=(rows,),
        in_specs=[
            pl.BlockSpec((1, width, samples, channels), lambda h: (h, 0, 0, 0)),
            pl.BlockSpec(table.shape, lambda h: (0, 0)),
        ],
        out_specs=tile_spec(dims),
        out_shape=pltpu.HBM((HALVES, split, GROUPS, local, rows, CK, HALF), BF16),
        compiler_params=params(16),
        cost_estimate=cost(3),
        name="columns",
    )(*far(x, table))


def columns_apart_kernel(at_ref, x_ref, t_ref, *refs):
    *outs, y_ref = refs
    y_ref[...] = column_modes(x_ref, t_ref).reshape(y_ref.shape)
    split, local = outs[0].shape[:2]
    for s in range(split * local):
        for a in range(HALVES):
            lanes = half_lanes(a ^ at_ref[1])
            for b in range(GROUPS):
                tile = y_ref[s * GROUPS + (b ^ at_ref[3]), :, lanes]
                outs[GROUPS * a + b][(s // local) ^ at_ref[2], s % local, 0] = tile


def columns_apart(at, x, table, dims):
    rows, width, samples, channels = x.shape
    split, local = dims
    out = pl.BlockSpec((split, local, 1, CK, HALF), lambda h, at: (0, 0, h, 0, 0))
    return pl.pallas_call(
        columns_apart_kernel,
        grid_spec=pltpu.PrefetchScalarGridSpec(
            num_scalar_prefetch=1,
            grid=(rows,),
            in_specs=[
                pl.BlockSpec((1, width, samples, channels), lambda h, at: (h, 0, 0, 0)),
                pl.BlockSpec(table.shape, lambda h, at: (0, 0)),
            ],
            out_specs=[out] * (HALVES * GROUPS),
            scratch_shapes=[pltpu.VMEM((samples * GROUPS, CK, channels), BF16)],
        ),
        out_shape=[pltpu.HBM((split, local, rows, CK, HALF), BF16)] * (HALVES * GROUPS),
        compiler_params=params(16),
        cost_estimate=cost(3),
        name="columns_apart",
    )(at, *far(x, table))


def add_modes(o_ref, x_ref, t_ref, z):
    _, width, samples, channels = x_ref.shape
    x = x_ref[0].reshape(width * samples, channels).astype(F32)
    o_ref[0] = (x + dot(t_ref[...], z)).astype(BF16).reshape(width, samples, channels)


def inverse_kernel(x_ref, t_ref, z_ref, o_ref):
    _, split, _, local = z_ref.shape[:4]
    z = jnp.concatenate(
        [
            jnp.concatenate(
                [
                    z_ref[half, s // local, :, s % local, 0].reshape(2 * MODES, HALF)
                    for half in range(HALVES)
                ],
                axis=1,
            )
            for s in range(split * local)
        ],
        axis=0,
    )
    add_modes(o_ref, x_ref, t_ref, z)


def inverse(x, table, z, dims):
    rows, width, samples, channels = x.shape
    whole = pl.BlockSpec((1, width, samples, channels), lambda h: (h, 0, 0, 0))
    return pl.pallas_call(
        inverse_kernel,
        grid=(rows,),
        in_specs=[whole, pl.BlockSpec(table.shape, lambda h: (0, 0)), tile_spec(dims)],
        out_specs=whole,
        out_shape=pltpu.HBM(x.shape, BF16),
        compiler_params=params(16),
        cost_estimate=cost(4),
        name="inverse",
    )(*far(x, table, z))


def inverse_apart_kernel(local, at_ref, x_ref, t_ref, *refs):
    *slabs, o_ref, z_ref = refs
    split = slabs[0].shape[0]
    row, rows = pl.program_id(0), pl.num_programs(0)
    for s in range(split * local):
        for a in range(HALVES):
            lanes = half_lanes(a ^ at_ref[1])
            for b in range(GROUPS):
                slab = slabs[GROUPS * a + b]
                tile = slab[(s // local) ^ at_ref[2], (s % local) * rows + row]
                z_ref[s * GROUPS + (b ^ at_ref[3]), :, lanes] = tile
    add_modes(o_ref, x_ref, t_ref, z_ref[...].reshape(t_ref.shape[1], x_ref.shape[3]))


def inverse_apart(at, x, table, slabs, dims):
    rows, width, samples, channels = x.shape
    whole = pl.BlockSpec((1, width, samples, channels), lambda h, at: (h, 0, 0, 0))
    return pl.pallas_call(
        functools.partial(inverse_apart_kernel, dims[1]),
        grid_spec=pltpu.PrefetchScalarGridSpec(
            num_scalar_prefetch=1,
            grid=(rows,),
            in_specs=[whole, pl.BlockSpec(table.shape, lambda h, at: (0, 0))]
            + [pl.BlockSpec(y.shape, lambda h, at: (0, 0, 0, 0)) for y in slabs],
            out_specs=whole,
            scratch_shapes=[pltpu.VMEM((samples * GROUPS, CK, channels), BF16)],
        ),
        out_shape=pltpu.HBM(x.shape, BF16),
        compiler_params=params(20),
        cost_estimate=cost(4),
        name="inverse_apart",
    )(at, *far(x, table, *slabs))


def transposed(out_ref, blocks):
    for j in range(0, len(blocks), 8):
        rows = jnp.concatenate([x.astype(F32) for x in blocks[j : j + 8]], axis=0)
        width = rows.shape[0]
        out_ref[:, (j // 8) * width : (j // 8 + 1) * width] = rows.T.astype(BF16)


def prepare_kernel(at_ref, base_ref, wi_ref, wo_ref, m_ref, mx_ref, nx_ref, *outs):
    shards = base_ref.shape[0]
    transposed(m_ref, [base_ref[r] for r in range(shards)])
    for r in range(shards):
        nx_ref[r] = base_ref[r ^ at_ref[0]]
    transposed(mx_ref, [nx_ref[r] for r in range(shards)])
    row = lax.broadcasted_iota(jnp.int32, (BLOCK, LANES), 0)
    lane = lax.broadcasted_iota(jnp.int32, (BLOCK, LANES), 1)
    place = jnp.where(lane == row, 1.0, 0.0).astype(BF16)
    below = jnp.zeros((LANES - BLOCK, LANES), F32)
    for w_ref, f_ref, t_ref in ((wi_ref, outs[0], outs[1]), (wo_ref, outs[2], outs[3])):
        for j in range(PER):
            real, imag = (
                jnp.concatenate([dot(w_ref[c, j], place), below], axis=0) for c in range(2)
            )
            real_t, imag_t = real.T.astype(BF16), imag.T.astype(BF16)
            real, imag = real.astype(BF16), imag.astype(BF16)
            f_ref[j, :LANES, :LANES] = real
            f_ref[j, :LANES, LANES:] = imag
            f_ref[j, LANES:, :LANES] = -imag
            f_ref[j, LANES:, LANES:] = real
            t_ref[j, :LANES, :LANES] = real_t
            t_ref[j, :LANES, LANES:] = -imag_t
            t_ref[j, LANES:, :LANES] = imag_t
            t_ref[j, LANES:, LANES:] = real_t


def prepare(at, base, in_weight, out_weight):
    blocks, rows, size = base.shape
    weight = pl.BlockSpec((2, HALF // BLOCK, BLOCK, BLOCK), lambda i, at: (0, at[1], 0, 0))
    square = pl.BlockSpec((size, size), lambda i, at: (0, 0))
    stack = pl.BlockSpec((blocks, rows, size), lambda i, at: (0, 0, 0))
    wide = pl.BlockSpec((PER, 2 * LANES, 2 * LANES), lambda i, at: (0, 0, 0))
    return pl.pallas_call(
        prepare_kernel,
        grid_spec=pltpu.PrefetchScalarGridSpec(
            num_scalar_prefetch=1,
            grid=(1,),
            in_specs=[stack, weight, weight],
            out_specs=[square, square, stack] + [wide] * 4,
        ),
        out_shape=[pltpu.HBM((size, size), BF16)] * 2
        + [pltpu.HBM((blocks, rows, size), BF16)]
        + [pltpu.HBM((PER, 2 * LANES, 2 * LANES), BF16)] * 4,
        compiler_params=params(40),
        cost_estimate=cost(4),
        name="prepare",
    )(at, base, in_weight, out_weight)


SLOPE = math.sqrt(2.0 / math.pi)


def padded(x):
    blank = jnp.zeros((x.shape[0], LANES - BLOCK), x.dtype)
    pieces = []
    for j in range(PER):
        pieces += [x[:, j * BLOCK : (j + 1) * BLOCK], blank]
    return jnp.concatenate(pieces, axis=1)


def packed(x):
    return jnp.concatenate([x[:, j * LANES : j * LANES + BLOCK] for j in range(PER)], axis=1)


def lanes_of(j):
    return slice(j * LANES, (j + 1) * LANES)


def parts_of(x, j):
    rows = x.shape[0] // 2
    return jnp.concatenate([x[:rows, lanes_of(j)], x[rows:, lanes_of(j)]], axis=1)


def joined(blocks):
    halves = [
        packed(jnp.concatenate([x[:, lanes_of(c)] for x in blocks], axis=1)) for c in range(2)
    ]
    return jnp.concatenate(halves, axis=0)


def bias_row(ref, j):
    return jnp.concatenate([ref[0:1, lanes_of(j)], ref[1:2, lanes_of(j)]], axis=1)


def forward_kernel(
    at_ref, v_ref, m_ref, n_ref, wi_ref, wo_ref, bi_ref, bo_ref, o_ref, s_ref, h_ref, d_ref
):
    del at_ref
    size = m_ref.shape[0]
    rows = size // 2
    spectrum = dot(m_ref[...], padded(v_ref[...].reshape(size, HALF))).astype(BF16)
    s_ref[0] = spectrum
    blocks = []
    for j in range(PER):
        pre = dot(parts_of(spectrum, j), wi_ref[j]) + bias_row(bi_ref, j)
        square = pre * pre
        tanh = jnp.tanh(SLOPE * (pre + 0.044715 * (square * pre)))
        gate = 0.5 * (1.0 + tanh)
        hidden = (pre * gate).astype(BF16)
        rise = SLOPE * (1.0 + 3 * 0.044715 * square)
        d_ref[0, j] = gate + 0.5 * pre * (1.0 - tanh * tanh) * rise
        h_ref[0, :rows, lanes_of(j)] = hidden[:, :LANES]
        h_ref[0, rows:, lanes_of(j)] = hidden[:, LANES:]
        blocks.append((dot(hidden, wo_ref[j]) + bias_row(bo_ref, j)).astype(BF16))
    back = dot(n_ref[...].reshape(size, size), joined(blocks)).astype(BF16)
    o_ref[...] = back.reshape(o_ref.shape)


def forward(rows, local, at, v, m, n, wi, wo, in_bias, out_bias):
    shards = v.shape[0]
    size = m.shape[0]
    chunk = pl.BlockSpec((shards, rows, CK, HALF), lambda s, at: (0, s, 0, 0))
    square = pl.BlockSpec((size, size), lambda s, at: (0, 0))
    stack = pl.BlockSpec(n.shape, lambda s, at: (0, 0, 0))
    wide = pl.BlockSpec((PER, 2 * LANES, 2 * LANES), lambda s, at: (0, 0, 0))
    bias = pl.BlockSpec((2, PER * LANES), lambda s, at: (0, at[1]))
    tall = pl.BlockSpec((1, size, PER * LANES), lambda s, at: (s, 0, 0))
    pair = pl.BlockSpec((1, PER, size // 2, 2 * LANES), lambda s, at: (s, 0, 0, 0))
    return pl.pallas_call(
        forward_kernel,
        grid_spec=pltpu.PrefetchScalarGridSpec(
            num_scalar_prefetch=1,
            grid=(local,),
            in_specs=[chunk, square, stack, wide, wide, bias, bias],
            out_specs=[chunk, tall, tall, pair],
        ),
        out_shape=[
            pltpu.HBM(v.shape, BF16),
            pltpu.HBM((local, size, PER * LANES), BF16),
            pltpu.HBM((local, size, PER * LANES), BF16),
            pltpu.HBM((local, PER, size // 2, 2 * LANES), F32),
        ],
        compiler_params=params(40),
        cost_estimate=cost(9),
        name="forward",
    )(at, *far(v, m, n, wi, wo, in_bias, out_bias))


PACK = 256


def outer_parts(p_ref, at, j, left, right):
    lanes = lanes_of(j)
    turned = jnp.concatenate([right[:, LANES:], -right[:, :LANES]], axis=1)
    full = dot_t(left, jnp.concatenate([right, turned], axis=0))
    sums = jnp.sum(right.astype(F32), axis=0, keepdims=True)
    for c in range(2):
        p_ref[at, c * BLOCK : (c + 1) * BLOCK, lanes] += full[:BLOCK, lanes_of(c)]
        p_ref[at, 2 * BLOCK + c : 2 * BLOCK + c + 1, lanes] += sums[:, lanes_of(c)]


def backward_kernel(at_ref, m_ref, wi_ref, wo_ref, s_ref, h_ref, d_ref, *refs):
    *slabs, g_ref, kept_ref, sent_ref, p_ref = refs

    @pl.when(pl.program_id(0) == 0)
    def _():
        p_ref[...] = jnp.zeros_like(p_ref)

    rows = slabs[0].shape[0] * CK
    v = jnp.concatenate([x[...].reshape(rows, HALF) for x in slabs], axis=0)
    incoming = dot(m_ref[...], padded(v)).astype(BF16)
    blocks = []
    for j in range(PER):
        coming = parts_of(incoming, j)
        pre_grad = (dot(coming, wo_ref[j]) * d_ref[0, j]).astype(BF16)
        blocks.append(dot(pre_grad, wi_ref[j]).astype(BF16))
        outer_parts(p_ref, 0, j, s_ref[0, :, lanes_of(j)], pre_grad)
        outer_parts(p_ref, 1, j, h_ref[0, :, lanes_of(j)], coming)
    g_ref[0] = joined(blocks)

    @pl.when(pl.program_id(0) == pl.num_programs(0) - 1)
    def _():
        kept_ref[...] = packed(p_ref[at_ref[4]])
        sent_ref[...] = packed(p_ref[1 - at_ref[4]])


def backward(rows, local, at, slabs, m, wi, wo, spectrum, hidden, slope):
    size = m.shape[0]
    slab = pl.BlockSpec((rows, CK, HALF), lambda s, at: (s, 0, 0))
    square = pl.BlockSpec((size, size), lambda s, at: (0, 0))
    wide = pl.BlockSpec((PER, 2 * LANES, 2 * LANES), lambda s, at: (0, 0, 0))
    tall = pl.BlockSpec((1, size, PER * LANES), lambda s, at: (s, 0, 0))
    given = pl.BlockSpec((1, size, HALF), lambda s, at: (s, 0, 0))
    pair = pl.BlockSpec((1, PER, size // 2, 2 * LANES), lambda s, at: (s, 0, 0, 0))
    packet = pl.BlockSpec((PACK, HALF), lambda s, at: (0, 0))
    return pl.pallas_call(
        backward_kernel,
        grid_spec=pltpu.PrefetchScalarGridSpec(
            num_scalar_prefetch=1,
            grid=(local,),
            in_specs=[square, wide, wide, tall, tall, pair] + [slab] * len(slabs),
            out_specs=[given, packet, packet],
            scratch_shapes=[pltpu.VMEM((2, PACK, PER * LANES), F32)],
        ),
        out_shape=[pltpu.HBM((local, size, HALF), BF16)] + [pltpu.HBM((PACK, HALF), F32)] * 2,
        compiler_params=params(40),
        cost_estimate=cost(9),
        name="backward",
    )(at, *far(m, wi, wo, spectrum, hidden, slope, *slabs))


def rows_back_kernel(at_ref, n_ref, g_ref, kept_ref, other_ref, *outs):
    blocks, rows, size = n_ref.shape
    local = g_ref.shape[0]
    both = jnp.concatenate([g_ref[s] for s in range(local)], axis=1)
    back = dot(n_ref[...].reshape(blocks * rows, size), both).astype(BF16)
    for s in range(local):
        part = back[:, s * HALF : (s + 1) * HALF].reshape(blocks, rows // CK, CK, HALF)
        for r in range(blocks):
            outs[r][s * rows // CK : (s + 1) * rows // CK] = part[r]
    tiles = local * rows // CK
    for r in range(blocks // HALVES):
        to = (r ^ at_ref[0]) % (blocks // HALVES)
        outs[r][tiles:] = (kept_ref[to] + other_ref[to]).astype(BF16)


def rows_back(at, n, grad, kept, other):
    blocks, rows, _ = n.shape
    tiles = grad.shape[0] * rows // CK
    counts = [tiles + kept.shape[1]] * (blocks // HALVES) + [tiles] * (blocks // HALVES)
    return pl.pallas_call(
        rows_back_kernel,
        in_specs=[pl.BlockSpec(memory_space=pltpu.SMEM)] + [pl.BlockSpec()] * 4,
        out_shape=[pltpu.HBM((count, CK, HALF), BF16) for count in counts],
        compiler_params=params(24),
        cost_estimate=cost(4),
        name="rows_back",
    )(at, *far(n, grad, kept, other))


def totals_kernel(*refs):
    *shares, o_ref = refs
    total = shares[0][...].astype(F32)
    for x in shares[1:]:
        total = total + x[...].astype(F32)
    total = total.astype(BF16)
    for t in range(o_ref.shape[0]):
        o_ref[t] = total


def totals(slabs, tiles):
    extra = slabs[0].shape[0] - tiles
    count = sum(x.shape[0] > tiles for x in slabs)
    shares = [
        pl.BlockSpec((1, CK, HALF), lambda i, t=t: (tiles + t, 0, 0)) for t in range(extra)
    ]
    body = totals_kernel
    if extra > 1:

        def body(*refs):
            *pieces, o_ref = refs
            for t in range(extra):
                totals_kernel(*pieces[t::extra], o_ref.at[:, t : t + 1])

    return pl.pallas_call(
        body,
        grid=(1,),
        in_specs=shares * count,
        out_specs=pl.BlockSpec((len(slabs), extra, CK, HALF), lambda i: (0, 0, 0, 0)),
        out_shape=pltpu.HBM((len(slabs), extra, CK, HALF), BF16),
        compiler_params=params(8),
        cost_estimate=cost(2),
        name="totals",
    )(*[y for y in far(*slabs[:count]) for _ in range(extra)])


def unpack_kernel(scale, at_ref, x_ref, y_ref, iw_ref, ib_ref, ow_ref, ob_ref, pack_ref):
    per = HALF // BLOCK
    for i, ref in enumerate((x_ref, y_ref)):
        count = ref.shape[0] // HALVES
        for half in range(HALVES):
            for place in range(count):
                block = ref[half * count + place].astype(F32) * scale
                pack_ref[i ^ at_ref[4], half, place] = block
    for mat, w_ref, b_ref in ((0, iw_ref, ib_ref), (1, ow_ref, ob_ref)):
        for half in range(HALVES):
            part = pack_ref[mat, half].reshape(PACK, HALF)
            for j in range(per):
                moved = part if j == 0 else pltpu.roll(part, HALF - j * BLOCK, 1)
                for c in range(2):
                    w_ref[c, half * per + j] = moved[c * BLOCK : (c + 1) * BLOCK, :BLOCK]
            b_ref[:, half * HALF : (half + 1) * HALF] = part[2 * BLOCK : 2 * BLOCK + 2]


def unpack(at, x, y, scale):
    weight = jax.ShapeDtypeStruct((2, BLOCKS, BLOCK, BLOCK), F32)
    bias = jax.ShapeDtypeStruct((2, HALVES * HALF), F32)
    return pl.pallas_call(
        functools.partial(unpack_kernel, scale),
        in_specs=[pl.BlockSpec(memory_space=pltpu.SMEM)]
        + [pl.BlockSpec(memory_space=pltpu.VMEM)] * 2,
        out_shape=[weight, bias, weight, bias],
        scratch_shapes=[pltpu.VMEM((2, HALVES, x.shape[0] // HALVES, *x.shape[1:]), F32)],
        compiler_params=params(16),
        cost_estimate=cost(2),
        name="unpack",
    )(at, x, y)


def unpack_joined(scale, packets):
    per = HALF // BLOCK
    out = []
    for mat in range(2):
        both = packets[mat].astype(F32) * scale
        weight = both[:, : 2 * BLOCK].reshape(HALVES, 2, BLOCK, per, BLOCK)
        out.append(weight.transpose(1, 0, 3, 2, 4).reshape(2, BLOCKS, BLOCK, BLOCK))
        out.append(both[:, 2 * BLOCK : 2 * BLOCK + 2].transpose(1, 0, 2).reshape(2, -1))
    return out


def swap(x, axis, size, bit):
    return lax.ppermute(x, axis, [(i, i ^ bit) for i in range(size)])


def bits_below(size):
    return [1 << b for b in range((size - 1).bit_length())]


def program(tokens, cotangent, in_weight, in_bias, out_weight, out_bias):
    samples, rows, width, _ = tokens.shape
    seq, rep = lax.axis_size("seq"), lax.axis_size("rep")
    split = seq // (HALVES * GROUPS)
    dims = (split, samples // split)
    local = dims[1]
    place, core = lax.axis_index("seq"), lax.axis_index("rep")
    at = jnp.stack(
        [
            place,
            place // (seq // HALVES),
            place // GROUPS % split,
            place % GROUPS,
            core // max(rep // 2, 1),
        ]
    ).astype(jnp.int32)
    plain, doubled = column_tables(width, samples)
    tokens, cotangent = (x.transpose(1, 2, 0, 3) for x in (tokens, cotangent))
    base = jnp.asarray(row_matrix(rows * seq).reshape(seq, rows * CK, -1), BF16)

    def table(t):
        return jnp.asarray(t, BF16)

    def exchange(x):
        return lax.all_to_all(x.reshape((seq, -1) + x.shape[-2:]), "seq", 0, 0, tiled=True)

    def apart(slabs):
        out = {0: slabs[0]}
        for r in range(1, seq):
            out[r] = swap(slabs[r], "seq", seq, r)
        return [out[r] for r in range(seq)]

    received = exchange(columns(tokens, table(plain), dims))
    cot = columns_apart(at, cotangent, table(doubled), dims)
    cot = [
        cot[GROUPS * a + b][c].reshape(local * rows, CK, HALF)
        for a in range(2)
        for c in range(split)
        for b in range(GROUPS)
    ]
    incoming = apart(cot)
    matrix, matrix_x, base_x, in_fwd, in_bwd, out_fwd, out_bwd = prepare(
        at, base, in_weight, out_weight
    )
    in_bias, out_bias = (
        jnp.pad(x.reshape(2, BLOCKS, BLOCK), ((0, 0), (0, 0), (0, LANES - BLOCK))).reshape(2, -1)
        for x in (in_bias, out_bias)
    )
    back, spectrum, hidden, slope = forward(
        rows, local, at, received, matrix, base, in_fwd, out_fwd, in_bias, out_bias
    )
    back = exchange(back)
    grad, kept, sent = backward(
        rows, local, at, incoming, matrix_x, in_bwd, out_bwd, spectrum, hidden, slope
    )

    bits = bits_below(rep)[::-1]
    other = swap(sent, "rep", rep, bits[0]) if bits else jnp.zeros_like(sent)
    for bit in bits[1:]:
        piece = kept + other
        count = piece.shape[0] // 2
        mine = (core // bit) % 2
        kept = lax.dynamic_slice_in_dim(piece, mine * count, count, 0)
        sent = lax.dynamic_slice_in_dim(piece, (1 - mine) * count, count, 0)
        other = swap(sent, "rep", rep, bit)
    part = kept.shape[0] * HALVES // seq
    whole_tiles = part % CK == 0

    def by_place(x):
        x = x.reshape(seq // HALVES, part, HALF)
        x = jnp.pad(x, ((0, 0), (0, -part % CK), (0, 0)))
        return x.reshape(seq // HALVES, -1, CK, HALF)

    grad = apart(rows_back(at, base_x, grad, by_place(kept), by_place(other)))
    near, back = lax.optimization_barrier((grad[: seq // HALVES], back))
    grad = near + grad[seq // HALVES :]
    total = totals(grad, local * rows)
    mixed_out = inverse(
        tokens,
        table(doubled.T),
        back.reshape(HALVES, split, GROUPS, local, rows, CK, HALF),
        dims,
    )
    gathered = exchange(total)
    slabs = [
        jnp.stack([grad[(a * split + c) * GROUPS + b] for c in range(split)])
        for a in range(2)
        for b in range(GROUPS)
    ]
    tokens_grad = inverse_apart(at, cotangent, table(plain.T), slabs, dims)
    gathered, tokens_grad = lax.optimization_barrier((gathered, tokens_grad))
    scale = 1.0 / (samples * rep)
    if rep == 2 and whole_tiles:
        gradients = unpack(at, gathered, swap(gathered, "rep", rep, 1), scale)
    else:
        piece = gathered.reshape(seq, -1, HALF)[:, :part].reshape(HALVES, -1, HALF)
        for bit in bits[::-1]:
            other = swap(piece, "rep", rep, bit)
            first = ((core // bit) % 2) == 0
            piece = jnp.concatenate(
                [jnp.where(first, piece, other), jnp.where(first, other, piece)], axis=1
            )
        packets = piece.reshape(HALVES, 2, PACK, HALF).transpose(1, 0, 2, 3)
        gradients = unpack_joined(scale, packets)
    mixed_out, tokens_grad = (x.transpose(2, 0, 1, 3) for x in (mixed_out, tokens_grad))
    return (mixed_out, tokens_grad, *gradients)


def solution(mesh):
    in_specs = (P("rep", "seq", None, None), P("rep", "seq", None, None), P(), P(), P(), P())
    out_specs = (P("rep", "seq", None, None), P("rep", "seq", None, None), P(), P(), P(), P())
    return jax.shard_map(program, mesh=mesh, in_specs=in_specs, out_specs=out_specs, check_vma=False)
```
